256 devices in a mesh: tm: 4 (over y, x), slab: 64 (over z, core).
Axes of the slice: x: 2, y: 2, z: 32, core: 2. Of those that a mesh axis runs over, the one named last changes fastest.
The devices are a block of a 4x8x32 slice.
Arguments:
- volumes: bfloat16 [32, 4096, 64, 128], P('tm', 'slab'), parts along dimension 0, may hold values from -6 to 6
- pair_fields: int32 [8, 1024], P(None, ('tm', 'slab')), parts along dimension 1, may hold values from -16 to 64, as said below
- pair_counts: int32 [256], P(('tm', 'slab')), parts along dimension 0, may hold values from 1 to 4, as said below
Outputs:
- correlation: float32 [1024, 512], P(('tm', 'slab')), parts along dimension 0
- shifts: float32 [3, 1024], P(None, ('tm', 'slab')), parts along dimension 1
- normal_sums: float32 [32, 4, 4], P('tm'), parts along dimension 0
- rhs_sums: float32 [32, 4, 3], P('tm'), parts along dimension 0
The draws below stay inside these ranges and needn't reach their ends.
There are 4 independent parts, one for each index of `tm`. The reference program is written for one: setup_inputs(seed, part) draws one part's arguments, and reference() takes and returns one part's arrays. A program takes and returns all parts, laid end to end along the dimension named above; each array names one. Nothing has to cross between parts.
Inputs may be any that keep to these rules, and one draw needn't show every extreme that they name: `pair_fields`: column p belongs to slab p // 4. Rows: first view; x anchor of its block (0 to 64); second view, the first plus or minus one modulo 8; slab offset of the second block (-1, 0 or 1, never leading outside the volume; 0 in dead columns); x anchor of the second block (0 to 64); window offsets along z, y, x (-16 to 8). Among one slab's live pairs at most 2 have slab offset 1 and at most 2 have -1; in every draw some slab has exactly 2 of each. The first pair of the first slab has slab offset 1 and the first pair of the last slab has -1. `pair_counts`: the live pairs of a slab fill its first slots; in every draw some slab has 4.
All inputs are finite; a program needn't handle non-finite values.
Results may differ from the reference program's by a relative error of at most 0.0003.
Values may be sent and summed in bfloat16 or wider, within the bound.
No kernel may reach another device: no remote copies, remote signals or barrier semaphores. Data moves between devices by JAX's collectives and lax.ppermute only.
A program may use at most 128 MiB of HBM per device.

```python
import jax
import jax.numpy as jnp
from jax import lax

VIEWS = 8
B = 64
WIN = 8
CAP = 4
NBR = 2
N_SLAB = 64


def pair_plan(key):
    base = jax.random.fold_in(key, 917)
    keys = jax.random.split(base, 9)
    slab_ids = jnp.arange(N_SLAB, dtype=jnp.int32)
    full_slab = jax.random.randint(keys[0], (), 1, N_SLAB - 1)
    heavy = jax.random.randint(keys[1], (N_SLAB,), 0, 8) == 0
    light = jax.random.randint(keys[2], (N_SLAB,), 1, CAP // 2 + 1)
    counts = jnp.where(heavy | (slab_ids == full_slab), CAP, light).astype(jnp.int32)
    pair_total = N_SLAB * CAP
    owner = jnp.arange(pair_total, dtype=jnp.int32) // CAP
    slot_index = jnp.arange(pair_total, dtype=jnp.int32) % CAP
    first_view = jax.random.randint(keys[3], (pair_total,), 0, VIEWS)
    step_sign = 2 * jax.random.randint(keys[4], (pair_total,), 0, 2) - 1
    second_view = jnp.mod(first_view + step_sign, VIEWS)
    first_x = jax.random.randint(keys[5], (pair_total,), 0, B + 1)
    second_x = jax.random.randint(keys[6], (pair_total,), 0, B + 1)
    offsets = jax.random.randint(keys[7], (3, pair_total), -2 * WIN, WIN + 1)
    direction = jax.random.randint(keys[8], (pair_total,), -1, 2)
    live = slot_index < counts[owner]
    direction = jnp.where(live, direction, 0)
    direction = jnp.where((owner == 0) & (direction < 0), 0, direction)
    direction = jnp.where((owner == N_SLAB - 1) & (direction > 0), 0, direction)
    direction = jnp.where((owner == 0) & (slot_index == 0), 1, direction)
    direction = jnp.where((owner == N_SLAB - 1) & (slot_index == 0), -1, direction)
    grid = direction.reshape(N_SLAB, CAP)
    up_rank = jnp.cumsum((grid == 1).astype(jnp.int32), axis=1)
    down_rank = jnp.cumsum((grid == -1).astype(jnp.int32), axis=1)
    grid = jnp.where((grid == 1) & (up_rank > NBR), 0, grid)
    grid = jnp.where((grid == -1) & (down_rank > NBR), 0, grid)
    slot_ids = jnp.arange(CAP, dtype=jnp.int32)
    forced = jnp.where(slot_ids < NBR, 1, jnp.where(slot_ids < 2 * NBR, -1, 0))
    grid = jnp.where((slab_ids == full_slab)[:, None], forced[None, :], grid)
    direction = grid.reshape(-1)
    fields = jnp.stack([first_view, first_x, second_view, direction, second_x, offsets[0], offsets[1], offsets[2]]).astype(jnp.int32)
    return (fields, counts)


def draw_pair_fields(key, part):
    return pair_plan(key)[0]


def draw_pair_counts(key, part):
    return pair_plan(key)[1]


def block_levels(rng, dims, shards, least, top_value):
    level, own = 1.0, jax.random.fold_in(rng, 6)
    for position, blocks in shards:
        draws = jnp.exp(jax.random.uniform(jax.random.fold_in(own, position), (blocks,), jnp.float32, least / len(shards), top_value / len(shards)))
        level = level * jnp.repeat(draws, dims[position] // blocks).reshape([-1 if axis == position else 1 for axis in range(len(dims))])
    return level


def centred(key, extent, scale, limit, cuts=(), held_as=jnp.bfloat16):
    loudness = block_levels(key, extent, cuts, -0.22, 0.18) if cuts else 1.0
    entries = jax.random.normal(key, extent, jnp.float32) * scale * loudness
    return jnp.minimum(jnp.maximum(entries, -limit), limit).astype(held_as)


def setup_inputs(seed: int = 0, part: int = 0) -> dict:
    arg_keys = jax.random.split(jax.random.key(seed), 4)
    own_keys = jax.random.split(jax.random.fold_in(arg_keys[3], part), 4)
    return {
        "volumes": centred(own_keys[0], (VIEWS, B * N_SLAB, B, 2 * B), 1.0, 6.0, ((1, 64),)),
        "pair_fields": draw_pair_fields(jax.random.fold_in(jax.random.fold_in(arg_keys[3], part), 71), part),
        "pair_counts": draw_pair_counts(jax.random.fold_in(jax.random.fold_in(arg_keys[3], part), 71), part),
    }


EPSILON = 1e-6


def reference(volumes, pair_fields, pair_counts):
    pair_total = CAP * N_SLAB
    window_steps = jnp.arange(WIN, dtype=jnp.int32)
    view_ids = jnp.arange(VIEWS, dtype=jnp.int32)

    def one_pair(pair_index):
        slab_pos = (pair_index // CAP).astype(jnp.int32)
        slot_index = pair_index % CAP
        column = pair_fields[:, pair_index]
        live_mask = (slot_index < pair_counts[slab_pos]).astype(jnp.float32)
        start_a = (slab_pos * B).astype(jnp.int32)
        start_b = ((slab_pos + column[3]) * B).astype(jnp.int32)
        block_a = lax.dynamic_slice(volumes, (column[0].astype(jnp.int32), start_a, jnp.zeros((), jnp.int32), column[1].astype(jnp.int32)), (1, B, B, B))[0].astype(jnp.float32)
        block_b = lax.dynamic_slice(volumes, (column[2].astype(jnp.int32), start_b, jnp.zeros((), jnp.int32), column[4].astype(jnp.int32)), (1, B, B, B))[0].astype(jnp.float32)
        spec_a = jnp.fft.fftn(block_a)
        spec_b = jnp.fft.fftn(block_b)
        cross_term = spec_a * jnp.conj(spec_b)
        magnitude = jnp.abs(cross_term)
        ratio_term = cross_term / (magnitude + (jnp.mean(magnitude) + EPSILON))
        full_corr = jnp.real(jnp.fft.ifftn(ratio_term)) * B ** 1.5
        idx_z = jnp.mod(column[5] + window_steps, B)
        idx_y = jnp.mod(column[6] + window_steps, B)
        idx_x = jnp.mod(column[7] + window_steps, B)
        values = full_corr[idx_z][:, idx_y][:, :, idx_x] * live_mask
        weight = values * values
        energy = jnp.mean(weight)
        steps_f = jnp.arange(WIN, dtype=jnp.float32)
        along_z = (column[5].astype(jnp.float32) + steps_f)[:, None, None]
        along_y = (column[6].astype(jnp.float32) + steps_f)[None, :, None]
        along_x = (column[7].astype(jnp.float32) + steps_f)[None, None, :]
        shift_vec = jnp.stack([jnp.mean(weight * along_z), jnp.mean(weight * along_y), jnp.mean(weight * along_x)]) / (energy + EPSILON)
        center = jnp.stack([
            (slab_pos.astype(jnp.float32) * B + 0.5 * B) / (B * N_SLAB),
            jnp.ones((), jnp.float32) * 0.5,
            (column[1].astype(jnp.float32) + 0.5 * B) / (2.0 * B),
            jnp.ones((), jnp.float32)])
        hit_a = (view_ids == column[0]).astype(jnp.float32)
        hit_b = (view_ids == column[2]).astype(jnp.float32)
        outer_hh = energy * center[:, None] * center[None, :]
        normal_part = (hit_a + hit_b)[:, None, None] * outer_hh[None]
        rhs_part = (hit_a - hit_b)[:, None, None] * (energy * center[:, None] * shift_vec[None, :])[None]
        return values.reshape(-1), shift_vec, normal_part, rhs_part

    corr_rows, shift_rows, normal_parts, rhs_parts = lax.map(one_pair, jnp.arange(pair_total, dtype=jnp.int32))
    normal_sums = jnp.sum(normal_parts, axis=0) / pair_total
    rhs_sums = jnp.sum(rhs_parts, axis=0) / pair_total
    return corr_rows, jnp.transpose(shift_rows), normal_sums, rhs_sums
```

```python
import math

import jax
import jax.numpy as jnp
import numpy as np
from jax import lax
from jax.experimental import pallas as pl
from jax.experimental.pallas import tpu as pltpu
from jax.sharding import PartitionSpec as P

WIN = 8
EPSILON = 1e-06
SLOTS = 4
EDGE = 64
HALF = 32
LANES = 128
ROWS = 8
XCHUNK = 8
F32 = jnp.float32
BF16 = jnp.bfloat16


def passed_along(value, axis, steps):
    count = lax.axis_size(axis)
    leading, last = (max(0, -steps), min(count, count - steps))
    return lax.ppermute(value, axis, [(source, source + steps) for source in range(leading, last)])


def basis_np():
    t = np.arange(EDGE)[:, None]
    s = np.arange(EDGE)[None, :]
    k = np.where(s <= HALF, s, s - HALF)
    angle = 2.0 * np.pi * ((k * t) % EDGE) / EDGE
    return np.where(s <= HALF, np.cos(angle), np.sin(angle))


def split_np(table):
    high = table.astype(BF16)
    low = (table - high.astype(np.float64)).astype(BF16)
    return high, low


def x_tables_np():
    table = basis_np()
    table = np.concatenate([table, table], axis=0)
    cos_part, sin_part = table[:, :HALF], table[:, HALF:]
    out = []
    for first, second in ((cos_part, sin_part), (sin_part, cos_part)):
        full = np.zeros((2 * LANES, LANES))
        for half in range(2):
            rows = slice(half * LANES, (half + 1) * LANES)
            full[rows, half * HALF : (half + 1) * HALF] = first
            full[rows, 2 * HALF + half * HALF : 2 * HALF + (half + 1) * HALF] = second
        out.append(np.concatenate(split_np(full), axis=1))
    return np.stack(out)


def y_table_np():
    high, low = split_np(basis_np().T)
    return np.concatenate([high, high, low], axis=1)


def split(values):
    high = values.astype(BF16)
    low = (values - high.astype(F32)).astype(BF16)
    return high, low


def times(value, angle_64):
    return value * float(np.float32(angle_64))


def rotate(re, im, phase):
    phase %= EDGE
    if phase == 0:
        return re, im
    c = math.cos(2.0 * math.pi * phase / EDGE)
    s = math.sin(2.0 * math.pi * phase / EDGE)
    if phase == EDGE // 4:
        return im, -re
    return times(re, c) + times(im, s), times(im, c) - times(re, s)


def real_dft8(x):
    r = math.sqrt(0.5)
    a0, a1, a2, a3 = x[0] + x[4], x[1] + x[5], x[2] + x[6], x[3] + x[7]
    b0, b1, b2, b3 = x[0] - x[4], x[1] - x[5], x[2] - x[6], x[3] - x[7]
    e0, e1 = a0 + a2, a1 + a3
    u, v = times(b1 - b3, r), times(b1 + b3, r)
    re = [e0 + e1, b0 + u, a0 - a2, b0 - u, e0 - e1]
    im = [None, -(b2 + v), a3 - a1, b2 - v, None]
    return re, im


def complex_dft4(re, im):
    a0r, a0i, a1r, a1i = re[0] + re[2], im[0] + im[2], re[0] - re[2], im[0] - im[2]
    b0r, b0i, b1r, b1i = re[1] + re[3], im[1] + im[3], re[1] - re[3], im[1] - im[3]
    return (
        [a0r + b0r, a1r + b1i, a0r - b0r, a1r - b1i],
        [a0i + b0i, a1i - b1r, a0i - b0i, a1i + b1r],
    )


def complex_dft8(re, im):
    er, ei = complex_dft4(re[0::2], im[0::2])
    odr, odi = complex_dft4(re[1::2], im[1::2])
    out_r, out_i = [None] * 8, [None] * 8
    for k in range(4):
        tr, ti = rotate(odr[k], odi[k], 8 * k)
        out_r[k], out_i[k] = er[k] + tr, ei[k] + ti
        out_r[k + 4], out_i[k + 4] = er[k] - tr, ei[k] - ti
    return out_r, out_i


def z_stage(grid_ref, column_ref):
    def column(index, carry):
        held = column_ref.at[index % 2]
        row = pl.multiple_of((index // 2) * ROWS, ROWS)
        lane = pl.multiple_of((index % 2) * LANES, LANES)

        def at(z):
            return grid_ref.at[z, pl.ds(row, ROWS), pl.ds(lane, LANES)]

        for z0 in range(8):
            re, im = real_dft8([at(8 * z1 + z0)[...] for z1 in range(8)])
            for n in range(5):
                held[8 * n + z0] = re[n]
            for n in range(1, 4):
                held[8 * (n + 4) + z0] = im[n]

        def keep(k, re, im):
            k %= EDGE
            if k > HALF:
                k, im = EDGE - k, -im
            at(k)[...] = re
            if k not in (0, HALF):
                at(HALF + k)[...] = -im

        re, im = real_dft8([held[z0] for z0 in range(8)])
        for n in range(5):
            keep(8 * n, re[n], im[n])
        y = [held[32 + z0] for z0 in range(8)]
        for first in (0, 1):
            sign = -1.0 if first == 0 else 1.0
            tr, ti = [], []
            for z0 in range(4):
                pr, pi = rotate(y[z0], sign * y[z0 + 4], 4 * z0 * (1 + 2 * first))
                tr.append(pr)
                ti.append(pi)
            dr, di = complex_dft4(tr, ti)
            keep(4 + 8 * first, dr[0], di[0])
            keep(4 + 8 * (first + 2), dr[1], di[1])
        for k1 in (1, 2, 3):
            re = [held[8 * k1 + z0] for z0 in range(8)]
            im = [held[8 * (k1 + 4) + z0] for z0 in range(8)]
            turned = [rotate(re[z0], im[z0], z0 * k1) for z0 in range(8)]
            dr, di = complex_dft8([p[0] for p in turned], [p[1] for p in turned])
            for k2 in range(8):
                keep(k1 + 8 * k2, dr[k2], di[k2])
        return carry

    lax.fori_loop(0, 2 * EDGE // ROWS, column, 0)


def masked_tables(table_ref, starts):
    out = []
    row = lax.broadcasted_iota(jnp.int32, (2 * LANES, 2 * LANES), 0)
    for part in range(2):
        low = jnp.where(row < LANES, starts[2 * part], starts[2 * part + 1])
        cell = row % LANES
        keep = (cell >= low) & (cell < low + EDGE)
        table = jnp.where(keep, table_ref[part].astype(F32), 0.0)
        out.append(table.astype(BF16))
    return out


def xy_stages(block_refs, wait_chunk, starts, x_table_ref, y_table_ref, masked_ref, grid_ref):
    for part, table in enumerate(masked_tables(x_table_ref, starts)):
        masked_ref[part] = table
    lane = lax.broadcasted_iota(jnp.int32, (XCHUNK * EDGE, LANES), 1)
    low_half = lane < EDGE

    def x_chunk(chunk, carry):
        first = chunk * XCHUNK
        wait_chunk(chunk)
        halves = []
        for part in range(2):
            rows = [
                block_refs[2 * part + k][pl.ds(first, XCHUNK)].reshape(XCHUNK * EDGE, LANES)
                for k in range(2)
            ]
            both = jnp.dot(
                jnp.concatenate(rows, axis=1), masked_ref[part], preferred_element_type=F32
            )
            halves.append(both[:, :LANES] + both[:, LANES:])
        cos_part = jnp.where(low_half, halves[0], halves[1])
        sin_part = pltpu.roll(jnp.where(low_half, halves[1], halves[0]), EDGE, 1)
        grid_ref[pl.ds(first, XCHUNK), :, :LANES] = cos_part.reshape(XCHUNK, EDGE, LANES)
        grid_ref[pl.ds(first, XCHUNK), :, LANES:] = sin_part.reshape(XCHUNK, EDGE, LANES)
        return carry

    lax.fori_loop(0, EDGE // XCHUNK, x_chunk, 0)

    def y_step(step, carry):
        for k in range(4):
            z = step * 4 + k
            high, low = split(grid_ref[z])
            grid_ref[z] = jnp.dot(
                y_table_ref[...],
                jnp.concatenate([high, low, high], axis=0),
                preferred_element_type=F32,
            )
        return carry

    lax.fori_loop(0, EDGE // 4, y_step, 0)


def zy_forward(cc, cs, sc, ss, z_zero, row_zero):
    if z_zero:
        return cc, cs, sc, ss
    r1, i1, r2, i2 = cc - ss, sc + cs, cc + ss, sc - cs
    if row_zero is not None:
        r1, i1 = jnp.where(row_zero, cc, r1), jnp.where(row_zero, sc, i1)
        r2, i2 = jnp.where(row_zero, cs, r2), jnp.where(row_zero, ss, i2)
    return r1, i1, r2, i2


def zy_adjoint(r1, i1, r2, i2, z_zero, row_zero):
    if z_zero:
        return r1, i1, r2, i2
    cc, cs, sc, ss = r1 + r2, i1 - i2, i1 + i2, r2 - r1
    if row_zero is not None:
        cc, sc = jnp.where(row_zero, r1, cc), jnp.where(row_zero, i1, sc)
        cs, ss = jnp.where(row_zero, r2, cs), jnp.where(row_zero, i2, ss)
    return cc, cs, sc, ss


def x_forward(rp, ip, rq, iq, lane_zero, row_zero):
    fa, fc = jnp.where(lane_zero, rp, rp - iq), jnp.where(lane_zero, ip, ip + rq)
    fb, fd = jnp.where(lane_zero, rq, rp + iq), jnp.where(lane_zero, iq, rq - ip)
    if row_zero is not None:
        fa, fc = jnp.where(row_zero, rp, fa), jnp.where(row_zero, rq, fc)
        fb, fd = jnp.where(row_zero, ip, fb), jnp.where(row_zero, iq, fd)
    return (fa, fc), (fb, fd)


def x_adjoint(first, second, lane_zero, row_zero):
    (ga, gc), (gb, gd) = first, second
    rp, iq = jnp.where(lane_zero, ga, ga + gb), jnp.where(lane_zero, gd, gb - ga)
    ip, rq = jnp.where(lane_zero, gc, gc - gd), jnp.where(lane_zero, gb, gc + gd)
    if row_zero is not None:
        rp, rq = jnp.where(row_zero, ga, rp), jnp.where(row_zero, gc, rq)
        ip, iq = jnp.where(row_zero, gb, ip), jnp.where(row_zero, gd, iq)
    return rp, ip, rq, iq


def octet(ref, kz, tile):
    row = tile * ROWS
    return [
        [
            ref.at[kz + dz, row + dy : row + dy + ROWS, lane : lane + LANES]
            for dz in (0, HALF)
            for dy in (0, HALF)
        ]
        for lane in (0, LANES)
    ]


def four_frequencies(ref, kz, tile, z_zero, lane_zero, row_zero):
    edge_row = row_zero if tile == 0 else None
    sides = []
    for pieces in octet(ref, kz, tile):
        cc, cs, sc, ss = [piece[...] for piece in pieces]
        sides.append(zy_forward(cc, cs, sc, ss, z_zero, edge_row))
    (rp1, ip1, rp2, ip2), (rq1, iq1, rq2, iq2) = sides
    corner_row = edge_row if z_zero else None
    return [
        *x_forward(rp1, ip1, rq1, iq1, lane_zero, corner_row),
        *x_forward(rp2, ip2, rq2, iq2, lane_zero, corner_row),
    ]


def cross_pass(grid_a, grid_b, size_ref, lane_zero, row_zero):
    corner = lane_zero & row_zero

    def one(kz, z_zero, total):
        for tile in range(4):
            fa = four_frequencies(grid_a, kz, tile, z_zero, lane_zero, row_zero)
            fb = four_frequencies(grid_b, kz, tile, z_zero, lane_zero, row_zero)
            pieces = [piece for side in octet(grid_b, kz, tile) for piece in side]
            for n in range(4):
                (ar, ai), (br, bi) = fa[n], fb[n]
                rr, ii = ar * br, ai * bi
                cr, ci = rr + ii, ai * br - ar * bi
                if z_zero and tile == 0:
                    cr, ci = jnp.where(corner, rr, cr), jnp.where(corner, ii, ci)
                size = jnp.sqrt(cr * cr + ci * ci)
                counted = size
                if z_zero and tile == 0:
                    counted = jnp.where(corner, 0.5 * (jnp.abs(cr) + jnp.abs(ci)), size)
                total = total + counted
                pieces[2 * n][...] = cr
                pieces[2 * n + 1][...] = ci
                size_ref[kz, tile, n] = size
        return total

    total = one(0, True, jnp.zeros((ROWS, LANES), F32))
    return lax.fori_loop(1, HALF, lambda kz, total: one(kz, False, total), total)


def ratio_pass(grid_b, size_ref, floor, lane_zero, row_zero):
    corner = lane_zero & row_zero

    def one(kz, z_zero):
        for tile in range(4):
            sides = octet(grid_b, kz, tile)
            pieces = [piece for side in sides for piece in side]
            ratios = []
            for n in range(4):
                cr, ci = pieces[2 * n][...], pieces[2 * n + 1][...]
                inverse = 1.0 / (size_ref[kz, tile, n] + floor)
                gr, gi = cr * inverse, ci * inverse
                if z_zero and tile == 0:
                    gr = jnp.where(corner, 0.5 * cr / (jnp.abs(cr) + floor), gr)
                    gi = jnp.where(corner, 0.5 * ci / (jnp.abs(ci) + floor), gi)
                ratios.append((gr, gi))
            edge_row = row_zero if tile == 0 else None
            corner_row = edge_row if z_zero else None
            rp1, ip1, rq1, iq1 = x_adjoint(ratios[0], ratios[1], lane_zero, corner_row)
            rp2, ip2, rq2, iq2 = x_adjoint(ratios[2], ratios[3], lane_zero, corner_row)
            for side, parts in zip(sides, ((rp1, ip1, rp2, ip2), (rq1, iq1, rq2, iq2))):
                for piece, value in zip(side, zy_adjoint(*parts, z_zero, edge_row)):
                    piece[...] = value

    one(0, True)

    def step(kz, carry):
        one(kz, False)
        return carry

    lax.fori_loop(1, HALF, step, 0)


def window_sums(grid_b, vy_ref, vz_ref, vx_ref):
    group = lax.broadcasted_iota(jnp.int32, (ROWS, 2 * LANES), 1) % LANES // HALF

    def step(number, carry):
        sums = list(carry)
        for k in range(2):
            sz = number * 2 + k
            high, low = split(grid_b[sz])
            mixed = jnp.dot(
                vy_ref[...], jnp.concatenate([high, low, high], axis=0), preferred_element_type=F32
            )
            rows = mixed[: WIN]
            for p in range(1, SLOTS):
                rows = jnp.where(group == p, mixed[p * WIN : (p + 1) * WIN], rows)
            for i in range(WIN):
                weight = jnp.broadcast_to(vz_ref[sz, i : i + 1, :], (ROWS, LANES))
                sums[2 * i] = sums[2 * i] + rows[:, :LANES] * weight
                sums[2 * i + 1] = sums[2 * i + 1] + rows[:, LANES:] * weight
        return tuple(sums)

    zero = jnp.zeros((ROWS, LANES), F32)
    sums = lax.fori_loop(0, EDGE // 2, step, (zero,) * (2 * WIN))
    stacked = jnp.concatenate(
        [jnp.concatenate([sums[2 * i], sums[2 * i + 1]], axis=1) for i in range(WIN)], axis=0
    )
    high, low = split(stacked)
    return jnp.dot(
        jnp.concatenate([high, low, high], axis=1), vx_ref[...], preferred_element_type=F32
    )


def first_kernel(fields, volumes_ref, x_table_ref, y_table_ref, out_ref, blocks, column, masked, sems):
    chunks = EDGE // XCHUNK

    def copy(p, chunk):
        view = fields[0, p]
        return pltpu.make_async_copy(
            volumes_ref.at[view, pl.ds(chunk * XCHUNK, XCHUNK)],
            blocks.at[p, pl.ds(chunk * XCHUNK, XCHUNK)],
            sems.at[p, chunk],
        )

    for chunk in range(chunks):
        for p in range(SLOTS):
            copy(p, chunk).start()

    def wait_chunk(chunk):
        for p in range(SLOTS):
            copy(p, chunk).wait()

    starts = [fields[1, p] for p in range(SLOTS)]
    xy_stages(
        [blocks.at[p] for p in range(SLOTS)],
        wait_chunk,
        starts,
        x_table_ref,
        y_table_ref,
        masked,
        out_ref,
    )
    z_stage(out_ref, column)


def rank_of(fields, slot, direction):
    rank = jnp.int32(0)
    for earlier in range(slot):
        rank = rank + (fields[3, earlier] == direction).astype(jnp.int32)
    return jnp.minimum(rank, 1)


def second_kernel(
    fields,
    counts,
    place,
    volumes_ref,
    above_ref,
    below_ref,
    grid_a_hbm,
    x_table_ref,
    y_table_ref,
    vy_ref,
    vz_ref,
    vx_ref,
    corr_ref,
    shift_ref,
    part_ref,
    blocks,
    grid_a,
    grid_b,
    sizes,
    column,
    masked,
    sems,
    a_sem,
):
    chunks = EDGE // XCHUNK
    a_copy = pltpu.make_async_copy(grid_a_hbm, grid_a, a_sem)

    def copy_from(source, p, chunk):
        return pltpu.make_async_copy(
            source.at[pl.ds(chunk * XCHUNK, XCHUNK)],
            blocks.at[p, pl.ds(chunk * XCHUNK, XCHUNK)],
            sems.at[p, chunk],
        )

    for chunk in range(chunks):
        for p in range(SLOTS):
            side = fields[3, p]
            for value, source in ((0, volumes_ref.at[fields[2, p]]), (1, above_ref), (-1, below_ref)):

                @pl.when(side == value)
                def _(source=source):
                    copy_from(source, p, chunk).start()

    a_copy.start()

    def wait_chunk(chunk):
        for p in range(SLOTS):
            copy_from(above_ref, p, chunk).wait()

    starts = []
    for p in range(SLOTS):
        side = fields[3, p]
        starts.append(jnp.where(side == 0, fields[4, p], EDGE * rank_of(fields, p, side)))
    xy_stages(
        [blocks.at[p] for p in range(SLOTS)],
        wait_chunk,
        starts,
        x_table_ref,
        y_table_ref,
        masked,
        grid_b,
    )
    z_stage(grid_b, column)
    a_copy.wait()
    lane = lax.broadcasted_iota(jnp.int32, (ROWS, LANES), 1)
    row = lax.broadcasted_iota(jnp.int32, (ROWS, LANES), 0)
    lane_zero, row_zero = lane % HALF == 0, row == 0
    total = cross_pass(grid_a, grid_b, sizes, lane_zero, row_zero)
    floor = jnp.zeros((1, LANES), F32)
    for p in range(SLOTS):
        mine = lane // HALF == p
        whole = jnp.sum(jnp.where(mine, total, 0.0), axis=(0, 1), keepdims=True)
        floor = jnp.where(mine[:1], whole * (2.0 / EDGE**3) + EPSILON, floor)
    floor = jnp.broadcast_to(floor, (ROWS, LANES))
    ratio_pass(grid_b, sizes, floor, lane_zero, row_zero)
    values = window_sums(grid_b, vy_ref, vz_ref, vx_ref)
    corr_ref[...] = values
    weight = values * values
    at = lax.broadcasted_iota(jnp.int32, (WIN * WIN, LANES), 0)
    along = [(at // WIN).astype(F32), (at % WIN).astype(F32)]
    k_row = (lane[:1] % WIN).astype(F32)
    plain = jnp.sum(weight, axis=0, keepdims=True)
    sums = [plain] + [jnp.sum(weight * a, axis=0, keepdims=True) for a in along] + [plain * k_row]
    stats = jnp.concatenate(sums + [jnp.zeros((ROWS - 4, LANES), F32)], axis=0) * (1.0 / WIN**3)
    for amount in (1, 2, 4):
        stats = stats + pltpu.roll(stats, LANES - amount, 1)
    shift_out = jnp.zeros((ROWS, LANES), F32)
    part = jnp.zeros((ROWS, LANES), F32)
    normal_lane = lane < 16
    first_of = jnp.where(normal_lane, lane // 4, (lane - 16) // 3)
    second_of = jnp.where(normal_lane, lane % 4, (lane - 16) % 3)
    edge = float(EDGE)
    slab_height = (place[0].astype(F32) * edge + 0.5 * edge) / (edge * place[1].astype(F32))
    for p in range(SLOTS):
        energy = stats[0:1, p * WIN : p * WIN + 1]
        moved = []
        for axis in range(3):
            first_moment = stats[axis + 1 : axis + 2, p * WIN : p * WIN + 1]
            moment = first_moment + energy * fields[5 + axis, p].astype(F32)
            moved.append(moment / (energy + EPSILON))
        anchor = (fields[1, p].astype(F32) + 0.5 * edge) / (2.0 * edge)

        def center(index):
            last = jnp.where(index == 2, anchor, 1.0)
            return jnp.where(index == 0, slab_height, jnp.where(index == 1, 0.5, last))

        moved_lane = jnp.where(
            second_of == 0, moved[0], jnp.where(second_of == 1, moved[1], moved[2])
        )
        other = jnp.where(normal_lane, center(second_of), moved_lane)
        hit_a = (row == fields[0, p]).astype(F32)
        hit_b = (row == fields[2, p]).astype(F32)
        hits = jnp.where(normal_lane, hit_a + hit_b, hit_a - hit_b)
        part = part + hits * (energy * center(first_of) * other)
        for axis in range(3):
            shift_out = jnp.where((lane == p) & (row == axis), moved[axis], shift_out)
    shift_ref[...] = shift_out
    part_ref[...] = jnp.where(lane < 28, part, 0.0)


def pick_view(fields, direction, rank):
    view = jnp.int32(0)
    seen = jnp.int32(0)
    for slot in range(SLOTS):
        asked = fields[3, slot] == direction
        view = jnp.where(asked & (seen == rank), fields[2, slot], view)
        seen = seen + asked.astype(jnp.int32)
    return view


def pick_start(fields, direction, rank):
    start = jnp.int32(0)
    seen = jnp.int32(0)
    for slot in range(SLOTS):
        asked = fields[3, slot] == direction
        start = jnp.where(asked & (seen == rank), fields[4, slot], start)
        seen = seen + asked.astype(jnp.int32)
    return start


def pack_kernel(below, above, b0_ref, b1_ref, a0_ref, a1_ref, down_ref, up_ref):
    planes = b0_ref.shape[1]
    lane = lax.broadcasted_iota(jnp.int32, (EDGE, LANES), 1)
    cell = lane % EDGE
    for fields, direction, first_ref, second_ref, out_ref in (
        (below, 1, b0_ref, b1_ref, down_ref),
        (above, -1, a0_ref, a1_ref, up_ref),
    ):
        plain_first = cell >= pick_start(fields, direction, 0)
        plain_second = cell < pick_start(fields, direction, 1)
        low_half = lane < EDGE
        keep = jnp.where(low_half, plain_first.astype(F32), plain_second.astype(F32)) > 0.0
        for z in range(planes):
            chosen = jnp.where(low_half, first_ref[0, z].astype(F32), second_ref[0, z].astype(F32))
            crossed = jnp.where(low_half, second_ref[0, z].astype(F32), first_ref[0, z].astype(F32))
            out_ref[z] = jnp.where(keep, chosen, pltpu.roll(crossed, EDGE, 1)).astype(BF16)


def packed_blocks(volumes, below_fields, above_fields):
    planes = 16
    block = (1, planes, EDGE, LANES)

    def taken(from_below, rank):
        def index(i, below, above):
            fields, direction = (below, 1) if from_below else (above, -1)
            return pick_view(fields, direction, rank), i, 0, 0

        return pl.BlockSpec(block, index)

    out_block = pl.BlockSpec((planes, EDGE, LANES), lambda i, below, above: (i, 0, 0))
    shape = jax.ShapeDtypeStruct((EDGE, EDGE, LANES), BF16)
    return pl.pallas_call(
        pack_kernel,
        out_shape=(shape, shape),
        grid_spec=pltpu.PrefetchScalarGridSpec(
            num_scalar_prefetch=2,
            grid=(EDGE // planes,),
            in_specs=[taken(True, 0), taken(True, 1), taken(False, 0), taken(False, 1)],
            out_specs=(out_block, out_block),
        ),
        name="pack",
    )(below_fields, above_fields, volumes, volumes, volumes, volumes)


def first_spectra(volumes, pair_fields, x_tables, y_table):
    whole = pl.BlockSpec(memory_space=pltpu.VMEM)
    return pl.pallas_call(
        first_kernel,
        out_shape=jax.ShapeDtypeStruct((EDGE, EDGE, 2 * LANES), F32),
        in_specs=[
            pl.BlockSpec(memory_space=pltpu.SMEM),
            pl.BlockSpec(memory_space=pl.ANY),
            whole,
            whole,
        ],
        out_specs=whole,
        scratch_shapes=[
            pltpu.VMEM((SLOTS, EDGE, EDGE, LANES), BF16),
            pltpu.VMEM((2, EDGE, ROWS, LANES), F32),
            pltpu.VMEM((2, 2 * LANES, 2 * LANES), BF16),
            pltpu.SemaphoreType.DMA((SLOTS, EDGE // XCHUNK)),
        ],
        name="first_spectra",
    )(pair_fields, volumes, x_tables, y_table)


def correlated(volumes, above, below, grid_a, pair_fields, pair_counts, place, tables):
    whole = pl.BlockSpec(memory_space=pltpu.VMEM)
    scalar = pl.BlockSpec(memory_space=pltpu.SMEM)
    left = pl.BlockSpec(memory_space=pl.ANY)
    grid = pltpu.VMEM((EDGE, EDGE, 2 * LANES), F32)
    return pl.pallas_call(
        second_kernel,
        out_shape=(
            jax.ShapeDtypeStruct((WIN * WIN, LANES), F32),
            jax.ShapeDtypeStruct((ROWS, LANES), F32),
            jax.ShapeDtypeStruct((ROWS, LANES), F32),
        ),
        in_specs=[scalar] * 3 + [left] * 4 + [whole] * 5,
        out_specs=(whole,) * 3,
        scratch_shapes=[
            pltpu.VMEM((SLOTS, EDGE, EDGE, LANES), BF16),
            grid,
            grid,
            pltpu.VMEM((HALF, 4, 4, ROWS, LANES), F32),
            pltpu.VMEM((2, EDGE, ROWS, LANES), F32),
            pltpu.VMEM((2, 2 * LANES, 2 * LANES), BF16),
            pltpu.SemaphoreType.DMA((SLOTS, EDGE // XCHUNK)),
            pltpu.SemaphoreType.DMA,
        ],
        name="correlated",
    )(pair_fields, pair_counts, place, volumes, above, below, grid_a, *tables)


def split_outside(values):
    high = lax.reduce_precision(values, 8, 7)
    return high.astype(BF16), (values - high).astype(BF16)


def window_tables(pair_fields, pair_counts):
    slot = jnp.arange(EDGE, dtype=jnp.int32)
    freq = jnp.where(slot <= HALF, slot, slot - HALF)
    steps = jnp.arange(WIN, dtype=jnp.int32)
    offsets = pair_fields[5:8] + jnp.array([[0], [0], [1]], jnp.int32) * (
        pair_fields[1] - pair_fields[4]
    )
    where_at = offsets[:, :, None, None] + steps[None, None, :, None]
    phase = jnp.mod(where_at * freq, EDGE) - jnp.where(slot <= HALF, 0, EDGE // 4)
    values = jnp.cos((2.0 * math.pi / EDGE) * phase.astype(F32))
    vz = jnp.repeat(jnp.transpose(values[0], (2, 1, 0)), HALF, axis=2)
    high, low = split_outside(values[1].reshape(SLOTS * WIN, EDGE))
    vy = jnp.concatenate([high, high, low], axis=1)
    live = (jnp.arange(SLOTS) < pair_counts[0]).astype(F32) * (2.0 / EDGE**1.5)
    vx = values[2] * live[:, None, None]
    vx = jnp.transpose(vx.reshape(SLOTS, WIN, 2, HALF), (2, 0, 3, 1))
    own = jnp.eye(SLOTS, dtype=F32)
    vx = (vx[:, :, :, None, :] * own[None, :, None, :, None]).reshape(2 * LANES, SLOTS * WIN)
    vx = jnp.pad(vx, ((0, 0), (0, LANES - SLOTS * WIN)))
    high, low = split_outside(vx)
    return vy, vz, jnp.concatenate([high, high, low], axis=0)


def group_sum(part, axis, size, stride):
    count = lax.axis_size(axis)
    groups = [
        [base + first + stride * k for k in range(size)]
        for base in range(0, count, size * stride)
        for first in range(stride)
    ]
    every = lax.all_gather(part, axis, axis=0, tiled=False, axis_index_groups=groups)
    return jnp.sum(every, axis=0)


def on_device(volumes, pair_fields, pair_counts):
    view_count = volumes.shape[0]
    slab_count = lax.axis_size("slab")
    own_index = lax.axis_index("slab")
    below_fields = passed_along(pair_fields, "slab", 1)
    above_fields = passed_along(pair_fields, "slab", -1)
    down, up = packed_blocks(volumes, below_fields, above_fields)
    from_above = passed_along(down, "slab", -1)
    from_below = passed_along(up, "slab", 1)
    x_tables, y_table = jnp.asarray(x_tables_np()), jnp.asarray(y_table_np())
    grid_a = first_spectra(volumes, pair_fields, x_tables, y_table)
    vy, vz, vx = window_tables(pair_fields, pair_counts)
    place = jnp.stack([own_index.astype(jnp.int32), jnp.int32(slab_count)])
    corr, shift, part = correlated(
        volumes,
        from_above,
        from_below,
        grid_a,
        pair_fields,
        pair_counts,
        place,
        (x_tables, y_table, vy, vz, vx),
    )
    corr = jnp.transpose(corr[:, : SLOTS * WIN].reshape(WIN * WIN, SLOTS, WIN), (1, 0, 2))
    corr = corr.reshape(SLOTS, WIN**3)
    first = 1
    while 2 * first * first <= slab_count:
        first *= 2
    while slab_count % first:
        first -= 1
    part = group_sum(part, "slab", first, 1)
    part = group_sum(part, "slab", slab_count // first, first)
    part = part * (1.0 / (SLOTS * slab_count))
    normal = part[:view_count, :16].reshape(view_count, 4, 4)
    rhs = part[:view_count, 16:28].reshape(view_count, 4, 3)
    return corr, shift[:3, :SLOTS], normal, rhs


def solution(mesh):
    in_specs = (P("tm", "slab", None, None), P(None, ("tm", "slab")), P(("tm", "slab")))
    out_specs = (
        P(("tm", "slab"), None),
        P(None, ("tm", "slab")),
        P("tm", None, None),
        P("tm", None, None),
    )
    return jax.shard_map(
        on_device, mesh=mesh, in_specs=in_specs, out_specs=out_specs, check_vma=False
    )
```

```python
import math

import jax
import jax.numpy as jnp
import numpy as np
from jax import lax
from jax.experimental import pallas as pl
from jax.experimental.pallas import tpu as pltpu
from jax.sharding import PartitionSpec as P

WIN = 8
EPSILON = 1e-06
SLOTS = 4
EDGE = 64
HALF = 32
LANES = 128
ROWS = 8
XCHUNK = 16
Y_UNROLL = 8
W_UNROLL = 8
PCHUNK = 8
GRANT = 24 << 20
F32 = jnp.float32
BF16 = jnp.bfloat16


def passed_along(value, axis, steps):
    count = lax.axis_size(axis)
    leading, last = (max(0, -steps), min(count, count - steps))
    return lax.ppermute(value, axis, [(source, source + steps) for source in range(leading, last)])


def basis_np():
    t = np.arange(EDGE)[:, None]
    s = np.arange(EDGE)[None, :]
    k = np.where(s <= HALF, s, s - HALF)
    angle = 2.0 * np.pi * ((k * t) % EDGE) / EDGE
    return np.where(s <= HALF, np.cos(angle), np.sin(angle))


def split_np(table):
    high = table.astype(BF16)
    low = (table - high.astype(np.float64)).astype(BF16)
    return high, low


def x_tables_np():
    table = basis_np()
    table = np.concatenate([table, table], axis=0)
    cos_part, sin_part = table[:, :HALF], table[:, HALF:]
    out = []
    for first, second in ((cos_part, sin_part), (sin_part, cos_part)):
        full = np.zeros((2 * LANES, LANES))
        for half in range(2):
            rows = slice(half * LANES, (half + 1) * LANES)
            full[rows, half * HALF : (half + 1) * HALF] = first
            full[rows, 2 * HALF + half * HALF : 2 * HALF + (half + 1) * HALF] = second
        out.append(np.concatenate(split_np(full), axis=1))
    return np.stack(out)


def y_table_np():
    high, low = split_np(basis_np().T)
    above = np.concatenate([high, high], axis=1)
    return np.concatenate([above, np.concatenate([low, np.zeros_like(low)], axis=1)], axis=0)


def split(values):
    high = values.astype(BF16)
    low = (values - high.astype(F32)).astype(BF16)
    return high, low


def times(value, angle_64):
    return value * float(np.float32(angle_64))


def rotate(re, im, phase):
    phase %= EDGE
    if phase == 0:
        return re, im
    c = math.cos(2.0 * math.pi * phase / EDGE)
    s = math.sin(2.0 * math.pi * phase / EDGE)
    if phase == EDGE // 4:
        return im, -re
    return times(re, c) + times(im, s), times(im, c) - times(re, s)


def real_dft8(x):
    r = math.sqrt(0.5)
    a0, a1, a2, a3 = x[0] + x[4], x[1] + x[5], x[2] + x[6], x[3] + x[7]
    b0, b1, b2, b3 = x[0] - x[4], x[1] - x[5], x[2] - x[6], x[3] - x[7]
    e0, e1 = a0 + a2, a1 + a3
    u, v = times(b1 - b3, r), times(b1 + b3, r)
    re = [e0 + e1, b0 + u, a0 - a2, b0 - u, e0 - e1]
    im = [None, -(b2 + v), a3 - a1, b2 - v, None]
    return re, im


def complex_dft4(re, im):
    a0r, a0i, a1r, a1i = re[0] + re[2], im[0] + im[2], re[0] - re[2], im[0] - im[2]
    b0r, b0i, b1r, b1i = re[1] + re[3], im[1] + im[3], re[1] - re[3], im[1] - im[3]
    return (
        [a0r + b0r, a1r + b1i, a0r - b0r, a1r - b1i],
        [a0i + b0i, a1i - b1r, a0i - b0i, a1i + b1r],
    )


def complex_dft8(re, im):
    er, ei = complex_dft4(re[0::2], im[0::2])
    odr, odi = complex_dft4(re[1::2], im[1::2])
    out_r, out_i = [None] * 8, [None] * 8
    for k in range(4):
        tr, ti = rotate(odr[k], odi[k], 8 * k)
        out_r[k], out_i[k] = er[k] + tr, ei[k] + ti
        out_r[k + 4], out_i[k + 4] = er[k] - tr, ei[k] - ti
    return out_r, out_i


def z_stage(grid_ref, column_ref):
    def column(index, carry):
        held = column_ref.at[index % 2]
        row = pl.multiple_of((index // 2) * ROWS, ROWS)
        lane = pl.multiple_of((index % 2) * LANES, LANES)

        def at(z):
            return grid_ref.at[z, pl.ds(row, ROWS), pl.ds(lane, LANES)]

        for z0 in range(8):
            re, im = real_dft8([at(8 * z1 + z0)[...] for z1 in range(8)])
            for n in range(5):
                held[8 * n + z0] = re[n]
            for n in range(1, 4):
                held[8 * (n + 4) + z0] = im[n]

        def keep(k, re, im):
            k %= EDGE
            if k > HALF:
                k, im = EDGE - k, -im
            at(k)[...] = re
            if k not in (0, HALF):
                at(HALF + k)[...] = -im

        re, im = real_dft8([held[z0] for z0 in range(8)])
        for n in range(5):
            keep(8 * n, re[n], im[n])
        y = [held[32 + z0] for z0 in range(8)]
        for first in (0, 1):
            sign = -1.0 if first == 0 else 1.0
            tr, ti = [], []
            for z0 in range(4):
                pr, pi = rotate(y[z0], sign * y[z0 + 4], 4 * z0 * (1 + 2 * first))
                tr.append(pr)
                ti.append(pi)
            dr, di = complex_dft4(tr, ti)
            keep(4 + 8 * first, dr[0], di[0])
            keep(4 + 8 * (first + 2), dr[1], di[1])
        for k1 in (1, 2, 3):
            re = [held[8 * k1 + z0] for z0 in range(8)]
            im = [held[8 * (k1 + 4) + z0] for z0 in range(8)]
            turned = [rotate(re[z0], im[z0], z0 * k1) for z0 in range(8)]
            dr, di = complex_dft8([p[0] for p in turned], [p[1] for p in turned])
            for k2 in range(8):
                keep(k1 + 8 * k2, dr[k2], di[k2])
        return carry

    lax.fori_loop(0, 2 * EDGE // ROWS, column, 0)


def masked_tables(table_ref, starts):
    out = []
    row = lax.broadcasted_iota(jnp.int32, (2 * LANES, 2 * LANES), 0)
    for part in range(2):
        low = jnp.where(row < LANES, starts[2 * part], starts[2 * part + 1])
        cell = row % LANES
        keep = (cell >= low) & (cell < low + EDGE)
        table = jnp.where(keep, table_ref[part].astype(F32), 0.0)
        out.append(table.astype(BF16))
    return out


def xy_stages(block_refs, wait_chunk, starts, x_table_ref, y_table_ref, masked_ref, grid_ref):
    for part, table in enumerate(masked_tables(x_table_ref, starts)):
        masked_ref[part] = table
    lane = lax.broadcasted_iota(jnp.int32, (XCHUNK * EDGE, LANES), 1)
    low_half = lane < EDGE

    def x_chunk(chunk, carry):
        first = chunk * XCHUNK
        wait_chunk(chunk)
        halves = []
        for part in range(2):
            rows = [
                block_refs[2 * part + k][pl.ds(first, XCHUNK)].reshape(XCHUNK * EDGE, LANES)
                for k in range(2)
            ]
            both = jnp.dot(
                jnp.concatenate(rows, axis=1), masked_ref[part], preferred_element_type=F32
            )
            halves.append(both[:, :LANES] + both[:, LANES:])
        cos_part = jnp.where(low_half, halves[0], halves[1])
        sin_part = pltpu.roll(jnp.where(low_half, halves[1], halves[0]), EDGE, 1)
        grid_ref[pl.ds(first, XCHUNK), :, :LANES] = cos_part.reshape(XCHUNK, EDGE, LANES)
        grid_ref[pl.ds(first, XCHUNK), :, LANES:] = sin_part.reshape(XCHUNK, EDGE, LANES)
        return carry

    lax.fori_loop(0, EDGE // XCHUNK, x_chunk, 0)

    def y_step(step, carry):
        for k in range(Y_UNROLL):
            z = step * Y_UNROLL + k
            high, low = split(grid_ref[z])
            both = jnp.dot(
                y_table_ref[...], jnp.concatenate([high, low], axis=0), preferred_element_type=F32
            )
            grid_ref[z] = both[:EDGE] + both[EDGE:]
        return carry

    lax.fori_loop(0, EDGE // Y_UNROLL, y_step, 0)


def zy_forward(cc, cs, sc, ss, z_zero, row_zero):
    if z_zero:
        return cc, cs, sc, ss
    r1, i1, r2, i2 = cc - ss, sc + cs, cc + ss, sc - cs
    if row_zero is not None:
        r1, i1 = jnp.where(row_zero, cc, r1), jnp.where(row_zero, sc, i1)
        r2, i2 = jnp.where(row_zero, cs, r2), jnp.where(row_zero, ss, i2)
    return r1, i1, r2, i2


def zy_adjoint(r1, i1, r2, i2, z_zero, row_zero):
    if z_zero:
        return r1, i1, r2, i2
    cc, cs, sc, ss = r1 + r2, i1 - i2, i1 + i2, r2 - r1
    if row_zero is not None:
        cc, sc = jnp.where(row_zero, r1, cc), jnp.where(row_zero, i1, sc)
        cs, ss = jnp.where(row_zero, r2, cs), jnp.where(row_zero, i2, ss)
    return cc, cs, sc, ss


def x_forward(rp, ip, rq, iq, lane_zero, row_zero):
    fa, fc = jnp.where(lane_zero, rp, rp - iq), jnp.where(lane_zero, ip, ip + rq)
    fb, fd = jnp.where(lane_zero, rq, rp + iq), jnp.where(lane_zero, iq, rq - ip)
    if row_zero is not None:
        fa, fc = jnp.where(row_zero, rp, fa), jnp.where(row_zero, rq, fc)
        fb, fd = jnp.where(row_zero, ip, fb), jnp.where(row_zero, iq, fd)
    return (fa, fc), (fb, fd)


def x_adjoint(first, second, lane_zero, row_zero):
    (ga, gc), (gb, gd) = first, second
    rp, iq = jnp.where(lane_zero, ga, ga + gb), jnp.where(lane_zero, gd, gb - ga)
    ip, rq = jnp.where(lane_zero, gc, gc - gd), jnp.where(lane_zero, gb, gc + gd)
    if row_zero is not None:
        rp, rq = jnp.where(row_zero, ga, rp), jnp.where(row_zero, gc, rq)
        ip, iq = jnp.where(row_zero, gb, ip), jnp.where(row_zero, gd, iq)
    return rp, ip, rq, iq


def octet(ref, kz, tile):
    row = tile * ROWS
    return [
        [
            ref.at[kz + dz, row + dy : row + dy + ROWS, lane : lane + LANES]
            for dz in (0, HALF)
            for dy in (0, HALF)
        ]
        for lane in (0, LANES)
    ]


def four_frequencies(ref, kz, tile, z_zero, lane_zero, row_zero):
    edge_row = row_zero if tile == 0 else None
    sides = []
    for pieces in octet(ref, kz, tile):
        cc, cs, sc, ss = [piece[...] for piece in pieces]
        sides.append(zy_forward(cc, cs, sc, ss, z_zero, edge_row))
    (rp1, ip1, rp2, ip2), (rq1, iq1, rq2, iq2) = sides
    corner_row = edge_row if z_zero else None
    return [
        *x_forward(rp1, ip1, rq1, iq1, lane_zero, corner_row),
        *x_forward(rp2, ip2, rq2, iq2, lane_zero, corner_row),
    ]


def cross_pass(grid_a, grid_b, size_ref, lane_zero, row_zero):
    corner = lane_zero & row_zero

    def one(kz, z_zero, total):
        for tile in range(4):
            fa = four_frequencies(grid_a, kz, tile, z_zero, lane_zero, row_zero)
            fb = four_frequencies(grid_b, kz, tile, z_zero, lane_zero, row_zero)
            pieces = [piece for side in octet(grid_b, kz, tile) for piece in side]
            for n in range(4):
                (ar, ai), (br, bi) = fa[n], fb[n]
                rr, ii = ar * br, ai * bi
                cr, ci = rr + ii, ai * br - ar * bi
                if z_zero and tile == 0:
                    cr, ci = jnp.where(corner, rr, cr), jnp.where(corner, ii, ci)
                size = jnp.sqrt(cr * cr + ci * ci)
                counted = size
                if z_zero and tile == 0:
                    counted = jnp.where(corner, 0.5 * (jnp.abs(cr) + jnp.abs(ci)), size)
                total = total + counted
                pieces[2 * n][...] = cr
                pieces[2 * n + 1][...] = ci
                size_ref[kz, tile, n] = size
        return total

    total = one(0, True, jnp.zeros((ROWS, LANES), F32))
    return lax.fori_loop(1, HALF, lambda kz, total: one(kz, False, total), total)


def ratio_pass(grid_b, size_ref, floor, lane_zero, row_zero):
    corner = lane_zero & row_zero

    def one(kz, z_zero):
        for tile in range(4):
            sides = octet(grid_b, kz, tile)
            pieces = [piece for side in sides for piece in side]
            ratios = []
            for n in range(4):
                cr, ci = pieces[2 * n][...], pieces[2 * n + 1][...]
                inverse = 1.0 / (size_ref[kz, tile, n] + floor)
                gr, gi = cr * inverse, ci * inverse
                if z_zero and tile == 0:
                    gr = jnp.where(corner, 0.5 * cr / (jnp.abs(cr) + floor), gr)
                    gi = jnp.where(corner, 0.5 * ci / (jnp.abs(ci) + floor), gi)
                ratios.append((gr, gi))
            edge_row = row_zero if tile == 0 else None
            corner_row = edge_row if z_zero else None
            rp1, ip1, rq1, iq1 = x_adjoint(ratios[0], ratios[1], lane_zero, corner_row)
            rp2, ip2, rq2, iq2 = x_adjoint(ratios[2], ratios[3], lane_zero, corner_row)
            for side, parts in zip(sides, ((rp1, ip1, rp2, ip2), (rq1, iq1, rq2, iq2))):
                for piece, value in zip(side, zy_adjoint(*parts, z_zero, edge_row)):
                    piece[...] = value

    one(0, True)

    def step(kz, carry):
        one(kz, False)
        return carry

    lax.fori_loop(1, HALF, step, 0)


def window_sums(grid_b, vy_ref, vz_ref, vx_ref):
    group = lax.broadcasted_iota(jnp.int32, (ROWS, 2 * LANES), 1) % LANES // HALF

    def step(number, carry):
        sums = list(carry)
        for k in range(W_UNROLL):
            sz = number * W_UNROLL + k
            high, low = split(grid_b[sz])
            both = jnp.dot(
                vy_ref[...], jnp.concatenate([high, low], axis=0), preferred_element_type=F32
            )
            mixed = both[: SLOTS * WIN] + both[SLOTS * WIN :]
            rows = mixed[: WIN]
            for p in range(1, SLOTS):
                rows = jnp.where(group == p, mixed[p * WIN : (p + 1) * WIN], rows)
            for i in range(WIN):
                weight = jnp.broadcast_to(vz_ref[sz, i : i + 1, :], (ROWS, LANES))
                sums[2 * i] = sums[2 * i] + rows[:, :LANES] * weight
                sums[2 * i + 1] = sums[2 * i + 1] + rows[:, LANES:] * weight
        return tuple(sums)

    zero = jnp.zeros((ROWS, LANES), F32)
    sums = lax.fori_loop(0, EDGE // W_UNROLL, step, (zero,) * (2 * WIN))
    stacked = jnp.concatenate(
        [jnp.concatenate([sums[2 * i], sums[2 * i + 1]], axis=1) for i in range(WIN)], axis=0
    )
    high, low = split(stacked)
    return jnp.dot(
        jnp.concatenate([high, low, high], axis=1), vx_ref[...], preferred_element_type=F32
    )


def flattened(values, flat_ref):
    rows, cols = WIN * WIN, WIN**3
    parts, left = [], values[:, : SLOTS * WIN]
    for _ in range(3):
        part = left.astype(BF16)
        parts.append(part)
        left = left - part.astype(F32)
    pair = lax.broadcasted_iota(jnp.int32, (rows, SLOTS * WIN), 1) // WIN
    own = lax.broadcasted_iota(jnp.int32, (rows, cols), 0)
    cell = lax.broadcasted_iota(jnp.int32, (rows, cols), 1) // WIN
    for p in range(SLOTS):
        mine = [jnp.where(pair == p, part.astype(F32), 0.0).astype(BF16) for part in parts]
        spread = jnp.dot(
            jnp.concatenate(mine, axis=1), flat_ref[...], preferred_element_type=F32
        )
        yield jnp.sum(jnp.where(own == cell, spread, 0.0), axis=0, keepdims=True)


def flat_table_np():
    row = np.arange(SLOTS * WIN)[:, None] % WIN
    col = np.arange(WIN**3)[None, :] % WIN
    return np.tile((row == col).astype(BF16), (3, 1))


def first_kernel(fields, volumes_ref, x_table_ref, y_table_ref, out_ref, blocks, column, masked, sems):
    chunks = EDGE // XCHUNK

    def copy(p, chunk):
        view = fields[p, 0]
        return pltpu.make_async_copy(
            volumes_ref.at[view, pl.ds(chunk * XCHUNK, XCHUNK)],
            blocks.at[p, pl.ds(chunk * XCHUNK, XCHUNK)],
            sems.at[p, chunk],
        )

    for chunk in range(chunks):
        for p in range(SLOTS):
            copy(p, chunk).start()

    def wait_chunk(chunk):
        for p in range(SLOTS):
            copy(p, chunk).wait()

    starts = [fields[p, 1] for p in range(SLOTS)]
    xy_stages(
        [blocks.at[p] for p in range(SLOTS)],
        wait_chunk,
        starts,
        x_table_ref,
        y_table_ref,
        masked,
        out_ref,
    )
    z_stage(out_ref, column)


def rank_of(fields, slot, direction):
    rank = jnp.int32(0)
    for earlier in range(slot):
        rank = rank + (fields[earlier, 3] == direction).astype(jnp.int32)
    return jnp.minimum(rank, 1)


def second_kernel(
    fields,
    volumes_ref,
    above_ref,
    below_ref,
    grid_a,
    x_table_ref,
    y_table_ref,
    vy_ref,
    vz_ref,
    vx_ref,
    flat_ref,
    corr_ref,
    shift_ref,
    part_ref,
    blocks,
    grid_b,
    sizes,
    column,
    masked,
    sems,
):
    chunks = EDGE // XCHUNK

    def copy_from(source, p, chunk):
        return pltpu.make_async_copy(
            source.at[pl.ds(chunk * XCHUNK, XCHUNK)],
            blocks.at[p, pl.ds(chunk * XCHUNK, XCHUNK)],
            sems.at[p, chunk],
        )

    for chunk in range(chunks):
        for p in range(SLOTS):
            side = fields[p, 3]
            for value, source in ((0, volumes_ref.at[fields[p, 2]]), (1, above_ref), (-1, below_ref)):

                @pl.when(side == value)
                def _(source=source):
                    copy_from(source, p, chunk).start()

    def wait_chunk(chunk):
        for p in range(SLOTS):
            copy_from(above_ref, p, chunk).wait()

    starts = []
    for p in range(SLOTS):
        side = fields[p, 3]
        starts.append(jnp.where(side == 0, fields[p, 4], EDGE * rank_of(fields, p, side)))
    xy_stages(
        [blocks.at[p] for p in range(SLOTS)],
        wait_chunk,
        starts,
        x_table_ref,
        y_table_ref,
        masked,
        grid_b,
    )
    z_stage(grid_b, column)
    lane = lax.broadcasted_iota(jnp.int32, (ROWS, LANES), 1)
    row = lax.broadcasted_iota(jnp.int32, (ROWS, LANES), 0)
    lane_zero, row_zero = lane % HALF == 0, row == 0
    total = cross_pass(grid_a, grid_b, sizes, lane_zero, row_zero)
    floor = jnp.zeros((1, LANES), F32)
    for p in range(SLOTS):
        mine = lane // HALF == p
        whole = jnp.sum(jnp.where(mine, total, 0.0), axis=(0, 1), keepdims=True)
        floor = jnp.where(mine[:1], whole * (2.0 / EDGE**3) + EPSILON, floor)
    floor = jnp.broadcast_to(floor, (ROWS, LANES))
    ratio_pass(grid_b, sizes, floor, lane_zero, row_zero)
    values = window_sums(grid_b, vy_ref, vz_ref, vx_ref)
    for p, line in enumerate(flattened(values, flat_ref)):
        corr_ref[p : p + 1, :] = line
    weight = values * values
    at = lax.broadcasted_iota(jnp.int32, (WIN * WIN, LANES), 0)
    along = [(at // WIN).astype(F32), (at % WIN).astype(F32)]
    k_row = (lane[:1] % WIN).astype(F32)
    plain = jnp.sum(weight, axis=0, keepdims=True)
    sums = [plain] + [jnp.sum(weight * a, axis=0, keepdims=True) for a in along] + [plain * k_row]
    stats = jnp.concatenate(sums + [jnp.zeros((ROWS - 4, LANES), F32)], axis=0) * (1.0 / WIN**3)
    for amount in (1, 2, 4):
        stats = stats + pltpu.roll(stats, LANES - amount, 1)
    shift_out = jnp.zeros((ROWS, LANES), F32)
    part = jnp.zeros((ROWS, LANES), F32)
    normal_lane = lane < 16
    first_of = jnp.where(normal_lane, lane // 4, lane % 4)
    second_of = jnp.where(normal_lane, lane % 4, (lane - 16) // 4)
    edge = float(EDGE)
    slab = lax.axis_index("slab").astype(F32)
    slab_height = (slab * edge + 0.5 * edge) / (edge * lax.axis_size("slab"))
    for p in range(SLOTS):
        energy = stats[0:1, p * WIN : p * WIN + 1]
        moved = []
        for axis in range(3):
            first_moment = stats[axis + 1 : axis + 2, p * WIN : p * WIN + 1]
            moment = first_moment + energy * fields[p, 5 + axis].astype(F32)
            moved.append(moment / (energy + EPSILON))
        anchor = (fields[p, 1].astype(F32) + 0.5 * edge) / (2.0 * edge)

        def center(index):
            last = jnp.where(index == 2, anchor, 1.0)
            return jnp.where(index == 0, slab_height, jnp.where(index == 1, 0.5, last))

        moved_lane = jnp.where(
            second_of == 0, moved[0], jnp.where(second_of == 1, moved[1], moved[2])
        )
        other = jnp.where(normal_lane, center(second_of), moved_lane)
        hit_a = (row == fields[p, 0]).astype(F32)
        hit_b = (row == fields[p, 2]).astype(F32)
        hits = jnp.where(normal_lane, hit_a + hit_b, hit_a - hit_b)
        part = part + hits * (energy * center(first_of) * other)
        for axis in range(3):
            shift_out = jnp.where((lane == p) & (row == axis), moved[axis], shift_out)
    shift_ref[...] = shift_out[:3, :SLOTS]
    part_ref[...] = jnp.where(lane < 28, part, 0.0)


def pick_view(fields, direction, rank):
    view = jnp.int32(0)
    seen = jnp.int32(0)
    for slot in range(SLOTS):
        asked = fields[slot, 3] == direction
        view = jnp.where(asked & (seen == rank), fields[slot, 2], view)
        seen = seen + asked.astype(jnp.int32)
    return view


def pick_start(fields, direction, rank):
    start = jnp.int32(0)
    seen = jnp.int32(0)
    for slot in range(SLOTS):
        asked = fields[slot, 3] == direction
        start = jnp.where(asked & (seen == rank), fields[slot, 4], start)
        seen = seen + asked.astype(jnp.int32)
    return start


def pack_kernel(below, above, volumes_ref, down_ref, up_ref, held, sems):
    lane = lax.broadcasted_iota(jnp.int32, (EDGE, LANES), 1)
    low_half = lane < EDGE
    sides = ((below, 1, down_ref), (above, -1, up_ref))
    views = [pick_view(fields, way, rank) for fields, way, _ in sides for rank in range(2)]

    def copy(n, chunk):
        return pltpu.make_async_copy(
            volumes_ref.at[views[n], pl.ds(chunk * PCHUNK, PCHUNK)],
            held.at[n, pl.ds(chunk * PCHUNK, PCHUNK)],
            sems.at[n, chunk],
        )

    for chunk in range(EDGE // PCHUNK):
        for n in range(4):
            copy(n, chunk).start()

    def weight(keep):
        return jnp.where(keep, 1.0, 0.0).astype(BF16)

    weights = []
    for fields, way, _ in sides:
        start_first, start_second = pick_start(fields, way, 0), pick_start(fields, way, 1)
        weights.append(
            (
                weight(low_half & (lane >= start_first)),
                weight(~low_half & (lane < start_second + EDGE)),
                weight(~low_half & (lane < start_first + EDGE)),
                weight(low_half & (lane >= start_second)),
            )
        )

    def step(chunk, carry):
        for n in range(4):
            copy(n, chunk).wait()
        for side, (_, _, out_ref) in enumerate(sides):
            stay_first, stay_second, move_first, move_second = weights[side]
            for k in range(PCHUNK):
                z = chunk * PCHUNK + k
                first, second = held[2 * side, z], held[2 * side + 1, z]
                moved = pltpu.roll(first * move_first + second * move_second, EDGE, 1)
                out_ref[z] = first * stay_first + second * stay_second + moved
        return carry

    lax.fori_loop(0, EDGE // PCHUNK, step, 0)


def packed_blocks(volumes, below_fields, above_fields):
    whole = pl.BlockSpec(memory_space=pltpu.VMEM)
    scalar = pl.BlockSpec(memory_space=pltpu.SMEM)
    shape = pltpu.VMEM((EDGE, EDGE, LANES), BF16)
    return pl.pallas_call(
        pack_kernel,
        out_shape=(shape, shape),
        in_specs=[scalar, scalar, pl.BlockSpec(memory_space=pl.ANY)],
        out_specs=(whole, whole),
        scratch_shapes=[
            pltpu.VMEM((4, EDGE, EDGE, LANES), BF16),
            pltpu.SemaphoreType.DMA((4, EDGE // PCHUNK)),
        ],
        compiler_params=pltpu.CompilerParams(vmem_limit_bytes=GRANT),
        name="pack",
    )(below_fields, above_fields, volumes)


def first_spectra(volumes, pair_fields, x_tables, y_table):
    whole = pl.BlockSpec(memory_space=pltpu.VMEM)
    return pl.pallas_call(
        first_kernel,
        out_shape=pltpu.VMEM((EDGE, EDGE, 2 * LANES), F32),
        in_specs=[
            pl.BlockSpec(memory_space=pltpu.SMEM),
            pl.BlockSpec(memory_space=pl.ANY),
            whole,
            whole,
        ],
        out_specs=whole,
        scratch_shapes=[
            pltpu.VMEM((SLOTS, EDGE, EDGE, LANES), BF16),
            pltpu.VMEM((2, EDGE, ROWS, LANES), F32),
            pltpu.VMEM((2, 2 * LANES, 2 * LANES), BF16),
            pltpu.SemaphoreType.DMA((SLOTS, EDGE // XCHUNK)),
        ],
        compiler_params=pltpu.CompilerParams(vmem_limit_bytes=GRANT),
        name="first_spectra",
    )(pair_fields, volumes, x_tables, y_table)


def correlated(volumes, above, below, grid_a, pair_fields, tables):
    whole = pl.BlockSpec(memory_space=pltpu.VMEM)
    scalar = pl.BlockSpec(memory_space=pltpu.SMEM)
    left = pl.BlockSpec(memory_space=pl.ANY)
    return pl.pallas_call(
        second_kernel,
        out_shape=(
            jax.ShapeDtypeStruct((SLOTS, WIN**3), F32),
            jax.ShapeDtypeStruct((3, SLOTS), F32),
            jax.ShapeDtypeStruct((ROWS, LANES), F32),
        ),
        in_specs=[scalar] + [left] * 3 + [whole] * 7,
        out_specs=(whole,) * 3,
        scratch_shapes=[
            pltpu.VMEM((SLOTS, EDGE, EDGE, LANES), BF16),
            pltpu.VMEM((EDGE, EDGE, 2 * LANES), F32),
            pltpu.VMEM((HALF, 4, 4, ROWS, LANES), F32),
            pltpu.VMEM((2, EDGE, ROWS, LANES), F32),
            pltpu.VMEM((2, 2 * LANES, 2 * LANES), BF16),
            pltpu.SemaphoreType.DMA((SLOTS, EDGE // XCHUNK)),
        ],
        compiler_params=pltpu.CompilerParams(vmem_limit_bytes=GRANT),
        name="correlated",
    )(pair_fields, volumes, above, below, grid_a, *tables)


def split_outside(values):
    high = lax.reduce_precision(values, 8, 7)
    return high.astype(BF16), (values - high).astype(BF16)


def window_tables(pair_fields, pair_counts):
    slot = jnp.arange(EDGE, dtype=jnp.int32)
    freq = jnp.where(slot <= HALF, slot, slot - HALF)
    steps = jnp.arange(WIN, dtype=jnp.int32)
    shift = pair_fields[:, 1:2] - pair_fields[:, 4:5]
    offsets = pair_fields[:, 5:8] + jnp.where(jnp.arange(3) == 2, shift, 0)
    where_at = jnp.transpose(offsets)[:, :, None, None] + steps[None, None, :, None]
    phase = jnp.mod(where_at * freq, EDGE) - jnp.where(slot <= HALF, 0, EDGE // 4)
    values = jnp.cos((2.0 * math.pi / EDGE) * phase.astype(F32))
    vz = jnp.repeat(jnp.transpose(values[0], (2, 1, 0)), HALF, axis=2)
    high, low = split_outside(values[1].reshape(SLOTS * WIN, EDGE))
    vy = jnp.concatenate(
        [
            jnp.concatenate([high, high], axis=1),
            jnp.concatenate([low, jnp.zeros_like(low)], axis=1),
        ],
        axis=0,
    )
    live = (jnp.arange(SLOTS) < pair_counts[0]).astype(F32) * (2.0 / EDGE**1.5)
    vx = values[2] * live[:, None, None]
    vx = jnp.transpose(vx.reshape(SLOTS, WIN, 2, HALF), (2, 0, 3, 1))
    own = jnp.eye(SLOTS, dtype=F32)
    vx = (vx[:, :, :, None, :] * own[None, :, None, :, None]).reshape(2 * LANES, SLOTS * WIN)
    vx = jnp.pad(vx, ((0, 0), (0, LANES - SLOTS * WIN)))
    high, low = split_outside(vx)
    return vy, vz, jnp.concatenate([high, high, low], axis=0)


def groups_of(count, size, stride):
    return [
        [base + first + stride * k for k in range(size)]
        for base in range(0, count, size * stride)
        for first in range(stride)
    ]


def slab_total(part, axis):
    count = lax.axis_size(axis)
    reach = 1
    for size in (2, 4):
        if count % (reach * size):
            break
        groups = groups_of(count, size, reach)
        if size == 2:
            part = jnp.sum(
                lax.all_gather(part, axis, axis=0, tiled=False, axis_index_groups=groups), axis=0
            )
        else:
            part = lax.psum(part, axis, axis_index_groups=groups)
        reach *= size
    if reach < count:
        part = lax.psum(part, axis, axis_index_groups=groups_of(count, count // reach, reach))
    return part


def on_device(volumes, pair_fields, pair_counts):
    view_count = volumes.shape[0]
    slab_count = lax.axis_size("slab")
    volumes = pltpu.with_memory_space_constraint(volumes, pltpu.HBM)
    pair_fields = jnp.transpose(pair_fields)
    below_fields = passed_along(pair_fields, "slab", 1)
    above_fields = passed_along(pair_fields, "slab", -1)
    down, up = packed_blocks(volumes, below_fields, above_fields)
    late_fields, late_counts, down, up = lax.optimization_barrier(
        (pair_fields, pair_counts, down, up)
    )
    from_above = pltpu.with_memory_space_constraint(passed_along(down, "slab", -1), pltpu.HBM)
    from_below = pltpu.with_memory_space_constraint(passed_along(up, "slab", 1), pltpu.HBM)
    x_tables, y_table = jnp.asarray(x_tables_np()), jnp.asarray(y_table_np())
    grid_a = first_spectra(volumes, late_fields, x_tables, y_table)
    windows = window_tables(late_fields, late_counts)
    corr, shift, part = correlated(
        volumes,
        from_above,
        from_below,
        grid_a,
        late_fields,
        (x_tables, y_table, *windows, jnp.asarray(flat_table_np())),
    )
    part = jnp.transpose(slab_total(part, "slab") * (1.0 / (SLOTS * slab_count)))
    normal = jnp.transpose(part[:16, :view_count].reshape(4, 4, view_count), (2, 0, 1))
    rhs = jnp.transpose(part[16:28, :view_count].reshape(3, 4, view_count), (2, 1, 0))
    return corr, shift, normal, rhs


def solution(mesh):
    in_specs = (P("tm", "slab", None, None), P(None, ("tm", "slab")), P(("tm", "slab")))
    out_specs = (
        P(("tm", "slab"), None),
        P(None, ("tm", "slab")),
        P("tm", None, None),
        P("tm", None, None),
    )
    return jax.shard_map(
        on_device, mesh=mesh, in_specs=in_specs, out_specs=out_specs, check_vma=False
    )
```

```python
import functools
import math

import jax
import jax.numpy as jnp
import numpy as np
from jax import lax
from jax.experimental import pallas as pl
from jax.experimental.pallas import tpu as pltpu
from jax.sharding import PartitionSpec as P


WIN = 8
EPSILON = 1e-06
TINY = 1e-37
SLOTS = 4
EDGE = 64
HALF = 32
LANES = 128
ROWS = 8
XCHUNK = 16
Y_UNROLL = 8
W_UNROLL = 8
PCHUNK = 8
GRANT = 24 << 20
F32 = jnp.float32
BF16 = jnp.bfloat16


def swapped(value, axis, first):
    pairs = [(low, low + 1) for low in range(first, lax.axis_size(axis) - 1, 2)]
    return lax.ppermute(value, axis, pairs + [(high, low) for low, high in pairs])


def partner_way():
    return 1 - 2 * (lax.axis_index("slab") % 2)


def basis_np():
    t = np.arange(EDGE)[:, None]
    s = np.arange(EDGE)[None, :]
    k = np.where(s <= HALF, s, s - HALF)
    angle = 2.0 * np.pi * ((k * t) % EDGE) / EDGE
    return np.where(s <= HALF, np.cos(angle), np.sin(angle))


def split_np(table):
    high = table.astype(BF16)
    low = (table - high.astype(np.float64)).astype(BF16)
    return high, low


def x_tables_np():
    table = basis_np()
    table = np.concatenate([table, table], axis=0)
    cos_part, sin_part = table[:, :HALF], table[:, HALF:]
    out = []
    for first, second in ((cos_part, sin_part), (sin_part, cos_part)):
        full = np.zeros((2 * LANES, LANES))
        for half in range(2):
            rows = slice(half * LANES, (half + 1) * LANES)
            full[rows, half * HALF : (half + 1) * HALF] = first
            full[rows, 2 * HALF + half * HALF : 2 * HALF + (half + 1) * HALF] = second
        out.append(np.concatenate(split_np(full), axis=1))
    return np.stack(out)


def y_table_np():
    high, low = split_np(basis_np().T)
    return np.concatenate([high, high, low], axis=1)


def split(values):
    high = values.astype(BF16)
    low = (values - high.astype(F32)).astype(BF16)
    return high, low


def times(value, angle_64):
    return value * float(np.float32(angle_64))


def rotate(re, im, phase):
    phase %= EDGE
    if phase == 0:
        return re, im
    c = math.cos(2.0 * math.pi * phase / EDGE)
    s = math.sin(2.0 * math.pi * phase / EDGE)
    if phase == EDGE // 4:
        return im, -re
    return times(re, c) + times(im, s), times(im, c) - times(re, s)


def real_dft8(x):
    r = math.sqrt(0.5)
    a0, a1, a2, a3 = x[0] + x[4], x[1] + x[5], x[2] + x[6], x[3] + x[7]
    b0, b1, b2, b3 = x[0] - x[4], x[1] - x[5], x[2] - x[6], x[3] - x[7]
    e0, e1 = a0 + a2, a1 + a3
    u, v = times(b1 - b3, r), times(b1 + b3, r)
    re = [e0 + e1, b0 + u, a0 - a2, b0 - u, e0 - e1]
    im = [None, -(b2 + v), a3 - a1, b2 - v, None]
    return re, im


def complex_dft4(re, im):
    a0r, a0i, a1r, a1i = re[0] + re[2], im[0] + im[2], re[0] - re[2], im[0] - im[2]
    b0r, b0i, b1r, b1i = re[1] + re[3], im[1] + im[3], re[1] - re[3], im[1] - im[3]
    return (
        [a0r + b0r, a1r + b1i, a0r - b0r, a1r - b1i],
        [a0i + b0i, a1i - b1r, a0i - b0i, a1i + b1r],
    )


def complex_dft8(re, im):
    er, ei = complex_dft4(re[0::2], im[0::2])
    odr, odi = complex_dft4(re[1::2], im[1::2])
    out_r, out_i = [None] * 8, [None] * 8
    for k in range(4):
        tr, ti = rotate(odr[k], odi[k], 8 * k)
        out_r[k], out_i[k] = er[k] + tr, ei[k] + ti
        out_r[k + 4], out_i[k + 4] = er[k] - tr, ei[k] - ti
    return out_r, out_i


def z_stage(grid_ref, column_ref):
    def column(index, carry):
        held = column_ref.at[index % 2]
        row = pl.multiple_of((index // 2) * ROWS, ROWS)
        lane = pl.multiple_of((index % 2) * LANES, LANES)

        def at(z):
            return grid_ref.at[z, pl.ds(row, ROWS), pl.ds(lane, LANES)]

        for z0 in range(8):
            re, im = real_dft8([at(8 * z1 + z0)[...] for z1 in range(8)])
            for n in range(5):
                held[8 * n + z0] = re[n]
            for n in range(1, 4):
                held[8 * (n + 4) + z0] = im[n]

        def keep(k, re, im):
            k %= EDGE
            if k > HALF:
                k, im = EDGE - k, -im
            at(k)[...] = re
            if k not in (0, HALF):
                at(HALF + k)[...] = -im

        re, im = real_dft8([held[z0] for z0 in range(8)])
        for n in range(5):
            keep(8 * n, re[n], im[n])
        y = [held[32 + z0] for z0 in range(8)]
        for first in (0, 1):
            sign = -1.0 if first == 0 else 1.0
            tr, ti = [], []
            for z0 in range(4):
                pr, pi = rotate(y[z0], sign * y[z0 + 4], 4 * z0 * (1 + 2 * first))
                tr.append(pr)
                ti.append(pi)
            dr, di = complex_dft4(tr, ti)
            keep(4 + 8 * first, dr[0], di[0])
            keep(4 + 8 * (first + 2), dr[1], di[1])
        for k1 in (1, 2, 3):
            re = [held[8 * k1 + z0] for z0 in range(8)]
            im = [held[8 * (k1 + 4) + z0] for z0 in range(8)]
            turned = [rotate(re[z0], im[z0], z0 * k1) for z0 in range(8)]
            dr, di = complex_dft8([p[0] for p in turned], [p[1] for p in turned])
            for k2 in range(8):
                keep(k1 + 8 * k2, dr[k2], di[k2])
        return carry

    lax.fori_loop(0, 2 * EDGE // ROWS, column, 0)


def masked_tables(table_ref, starts):
    out = []
    row = lax.broadcasted_iota(jnp.int32, (2 * LANES, 2 * LANES), 0)
    for part in range(2):
        low = jnp.where(row < LANES, starts[2 * part], starts[2 * part + 1])
        cell = row % LANES
        keep = (cell >= low) & (cell < low + EDGE)
        table = jnp.where(keep, table_ref[part].astype(F32), 0.0)
        out.append(table.astype(BF16))
    return out


def xy_stages(block_refs, wait_chunk, starts, x_table_ref, y_table_ref, masked_ref, grid_ref):
    for part, table in enumerate(masked_tables(x_table_ref, starts)):
        masked_ref[part] = table
    lane = lax.broadcasted_iota(jnp.int32, (XCHUNK * EDGE, LANES), 1)
    low_half = lane < EDGE

    def x_chunk(chunk, carry):
        first = chunk * XCHUNK
        wait_chunk(chunk)
        halves = []
        for part in range(2):
            rows = [
                block_refs[2 * part + k][pl.ds(first, XCHUNK)].reshape(XCHUNK * EDGE, LANES)
                for k in range(2)
            ]
            both = jnp.dot(
                jnp.concatenate(rows, axis=1), masked_ref[part], preferred_element_type=F32
            )
            halves.append(both[:, :LANES] + both[:, LANES:])
        cos_part = jnp.where(low_half, halves[0], halves[1])
        sin_part = pltpu.roll(jnp.where(low_half, halves[1], halves[0]), EDGE, 1)
        grid_ref[pl.ds(first, XCHUNK), :, :LANES] = cos_part.reshape(XCHUNK, EDGE, LANES)
        grid_ref[pl.ds(first, XCHUNK), :, LANES:] = sin_part.reshape(XCHUNK, EDGE, LANES)
        return carry

    lax.fori_loop(0, EDGE // XCHUNK, x_chunk, 0)

    def y_step(step, carry):
        for k in range(Y_UNROLL):
            z = step * Y_UNROLL + k
            high, low = split(grid_ref[z])
            grid_ref[z] = jnp.dot(
                y_table_ref[...],
                jnp.concatenate([high, low, high], axis=0),
                preferred_element_type=F32,
            )
        return carry

    lax.fori_loop(0, EDGE // Y_UNROLL, y_step, 0)


def zy_forward(cc, cs, sc, ss, z_zero, row_zero):
    if z_zero:
        return cc, cs, sc, ss
    r1, i1, r2, i2 = cc - ss, sc + cs, cc + ss, sc - cs
    if row_zero is not None:
        r1, i1 = jnp.where(row_zero, cc, r1), jnp.where(row_zero, sc, i1)
        r2, i2 = jnp.where(row_zero, cs, r2), jnp.where(row_zero, ss, i2)
    return r1, i1, r2, i2


def zy_adjoint(r1, i1, r2, i2, z_zero, row_zero):
    if z_zero:
        return r1, i1, r2, i2
    cc, cs, sc, ss = r1 + r2, i1 - i2, i1 + i2, r2 - r1
    if row_zero is not None:
        cc, sc = jnp.where(row_zero, r1, cc), jnp.where(row_zero, i1, sc)
        cs, ss = jnp.where(row_zero, r2, cs), jnp.where(row_zero, i2, ss)
    return cc, cs, sc, ss


def x_forward(rp, ip, rq, iq, lane_zero, row_zero):
    fa, fc = jnp.where(lane_zero, rp, rp - iq), jnp.where(lane_zero, ip, ip + rq)
    fb, fd = jnp.where(lane_zero, rq, rp + iq), jnp.where(lane_zero, iq, rq - ip)
    if row_zero is not None:
        fa, fc = jnp.where(row_zero, rp, fa), jnp.where(row_zero, rq, fc)
        fb, fd = jnp.where(row_zero, ip, fb), jnp.where(row_zero, iq, fd)
    return (fa, fc), (fb, fd)


def x_adjoint(first, second, lane_zero, row_zero):
    (ga, gc), (gb, gd) = first, second
    rp, iq = jnp.where(lane_zero, ga, ga + gb), jnp.where(lane_zero, gd, gb - ga)
    ip, rq = jnp.where(lane_zero, gc, gc - gd), jnp.where(lane_zero, gb, gc + gd)
    if row_zero is not None:
        rp, rq = jnp.where(row_zero, ga, rp), jnp.where(row_zero, gc, rq)
        ip, iq = jnp.where(row_zero, gb, ip), jnp.where(row_zero, gd, iq)
    return rp, ip, rq, iq


def octet(ref, kz, tile):
    row = tile * ROWS
    return [
        [
            ref.at[kz + dz, row + dy : row + dy + ROWS, lane : lane + LANES]
            for dz in (0, HALF)
            for dy in (0, HALF)
        ]
        for lane in (0, LANES)
    ]


def four_frequencies(ref, kz, tile, z_zero, lane_zero, row_zero):
    edge_row = row_zero if tile == 0 else None
    sides = []
    for pieces in octet(ref, kz, tile):
        cc, cs, sc, ss = [piece[...] for piece in pieces]
        sides.append(zy_forward(cc, cs, sc, ss, z_zero, edge_row))
    (rp1, ip1, rp2, ip2), (rq1, iq1, rq2, iq2) = sides
    corner_row = edge_row if z_zero else None
    return [
        *x_forward(rp1, ip1, rq1, iq1, lane_zero, corner_row),
        *x_forward(rp2, ip2, rq2, iq2, lane_zero, corner_row),
    ]


def cross_pass(grid_a, grid_b, size_ref, lane_zero, row_zero):
    corner = lane_zero & row_zero

    def one(kz, z_zero, total):
        for tile in range(4):
            fa = four_frequencies(grid_a, kz, tile, z_zero, lane_zero, row_zero)
            fb = four_frequencies(grid_b, kz, tile, z_zero, lane_zero, row_zero)
            pieces = [piece for side in octet(grid_b, kz, tile) for piece in side]
            for n in range(4):
                (ar, ai), (br, bi) = fa[n], fb[n]
                rr, ii = ar * br, ai * bi
                cr, ci = rr + ii, ai * br - ar * bi
                if z_zero and tile == 0:
                    cr, ci = jnp.where(corner, rr, cr), jnp.where(corner, ii, ci)
                square = cr * cr + ci * ci
                size = square * lax.rsqrt(jnp.maximum(square, TINY))
                counted = size
                if z_zero and tile == 0:
                    counted = jnp.where(corner, 0.5 * (jnp.abs(cr) + jnp.abs(ci)), size)
                total = total + counted
                pieces[2 * n][...] = cr
                pieces[2 * n + 1][...] = ci
                size_ref[kz, tile, n] = size
        return total

    total = one(0, True, jnp.zeros((ROWS, LANES), F32))
    return lax.fori_loop(1, HALF, lambda kz, total: one(kz, False, total), total)


def ratio_pass(grid_b, size_ref, floor, lane_zero, row_zero):
    corner = lane_zero & row_zero

    def one(kz, z_zero):
        for tile in range(4):
            sides = octet(grid_b, kz, tile)
            pieces = [piece for side in sides for piece in side]
            ratios = []
            for n in range(4):
                cr, ci = pieces[2 * n][...], pieces[2 * n + 1][...]
                inverse = 1.0 / (size_ref[kz, tile, n] + floor)
                gr, gi = cr * inverse, ci * inverse
                if z_zero and tile == 0:
                    gr = jnp.where(corner, 0.5 * cr / (jnp.abs(cr) + floor), gr)
                    gi = jnp.where(corner, 0.5 * ci / (jnp.abs(ci) + floor), gi)
                ratios.append((gr, gi))
            edge_row = row_zero if tile == 0 else None
            corner_row = edge_row if z_zero else None
            rp1, ip1, rq1, iq1 = x_adjoint(ratios[0], ratios[1], lane_zero, corner_row)
            rp2, ip2, rq2, iq2 = x_adjoint(ratios[2], ratios[3], lane_zero, corner_row)
            for side, parts in zip(sides, ((rp1, ip1, rp2, ip2), (rq1, iq1, rq2, iq2))):
                for piece, value in zip(side, zy_adjoint(*parts, z_zero, edge_row)):
                    piece[...] = value

    one(0, True)

    def step(kz, carry):
        one(kz, False)
        return carry

    lax.fori_loop(1, HALF, step, 0)


def window_sums(grid_b, vy_ref, vz_ref, vx_ref):
    group = lax.broadcasted_iota(jnp.int32, (ROWS, 2 * LANES), 1) % LANES // HALF

    def step(number, carry):
        sums = list(carry)
        for k in range(W_UNROLL):
            sz = number * W_UNROLL + k
            high, low = split(grid_b[sz])
            both = jnp.dot(
                vy_ref[...], jnp.concatenate([high, low], axis=0), preferred_element_type=F32
            )
            mixed = both[: SLOTS * WIN] + both[SLOTS * WIN :]
            rows = mixed[: WIN]
            for p in range(1, SLOTS):
                rows = jnp.where(group == p, mixed[p * WIN : (p + 1) * WIN], rows)
            for i in range(WIN):
                weight = jnp.broadcast_to(vz_ref[sz, i : i + 1, :], (ROWS, LANES))
                sums[2 * i] = sums[2 * i] + rows[:, :LANES] * weight
                sums[2 * i + 1] = sums[2 * i + 1] + rows[:, LANES:] * weight
        return tuple(sums)

    zero = jnp.zeros((ROWS, LANES), F32)
    sums = lax.fori_loop(0, EDGE // W_UNROLL, step, (zero,) * (2 * WIN))
    stacked = jnp.concatenate(
        [jnp.concatenate([sums[2 * i], sums[2 * i + 1]], axis=1) for i in range(WIN)], axis=0
    )
    high, low = split(stacked)
    return jnp.dot(
        jnp.concatenate([high, low, high], axis=1), vx_ref[...], preferred_element_type=F32
    )


def flattened(values, flat_ref):
    rows, cols = WIN * WIN, WIN**3
    parts, left = [], values[:, : SLOTS * WIN]
    for _ in range(3):
        part = left.astype(BF16)
        parts.append(part)
        left = left - part.astype(F32)
    pair = lax.broadcasted_iota(jnp.int32, (rows, SLOTS * WIN), 1) // WIN
    own = lax.broadcasted_iota(jnp.int32, (rows, cols), 0)
    cell = lax.broadcasted_iota(jnp.int32, (rows, cols), 1) // WIN
    for p in range(SLOTS):
        mine = [jnp.where(pair == p, part.astype(F32), 0.0).astype(BF16) for part in parts]
        spread = jnp.dot(
            jnp.concatenate(mine, axis=1), flat_ref[...], preferred_element_type=F32
        )
        yield jnp.sum(jnp.where(own == cell, spread, 0.0), axis=0, keepdims=True)


def flat_table_np():
    row = np.arange(SLOTS * WIN)[:, None] % WIN
    col = np.arange(WIN**3)[None, :] % WIN
    return np.tile((row == col).astype(BF16), (3, 1))


def first_kernel(fields, volumes_ref, x_table_ref, y_table_ref, out_ref, blocks, column, masked, sems):
    chunks = EDGE // XCHUNK

    def copy(p, chunk):
        view = fields[p, 0]
        return pltpu.make_async_copy(
            volumes_ref.at[view, pl.ds(chunk * XCHUNK, XCHUNK)],
            blocks.at[p, pl.ds(chunk * XCHUNK, XCHUNK)],
            sems.at[p, chunk],
        )

    for chunk in range(chunks):
        for p in range(SLOTS):
            copy(p, chunk).start()

    def wait_chunk(chunk):
        for p in range(SLOTS):
            copy(p, chunk).wait()

    starts = [fields[p, 1] for p in range(SLOTS)]
    xy_stages(
        [blocks.at[p] for p in range(SLOTS)],
        wait_chunk,
        starts,
        x_table_ref,
        y_table_ref,
        masked,
        out_ref,
    )
    z_stage(out_ref, column)


def rank_of(fields, slot, direction):
    rank = jnp.int32(0)
    for earlier in range(slot):
        rank = rank + (fields[earlier, 3] == direction).astype(jnp.int32)
    return jnp.minimum(rank, 1)


def second_kernel(
    fields,
    volumes_ref,
    partner_ref,
    cross_ref,
    grid_a,
    x_table_ref,
    y_table_ref,
    vy_ref,
    vz_ref,
    vx_ref,
    flat_ref,
    corr_ref,
    shift_ref,
    part_ref,
    blocks,
    grid_b,
    sizes,
    column,
    masked,
    sems,
):
    chunks = EDGE // XCHUNK

    def copy_from(source, p, chunk):
        return pltpu.make_async_copy(
            source.at[pl.ds(chunk * XCHUNK, XCHUNK)],
            blocks.at[p, pl.ds(chunk * XCHUNK, XCHUNK)],
            sems.at[p, chunk],
        )

    way = partner_way()
    for chunk in range(chunks):
        for p in range(SLOTS):
            side = fields[p, 3]
            local = volumes_ref.at[fields[p, 2]]
            for value, source in ((0, local), (way, partner_ref), (-way, cross_ref)):

                @pl.when(side == value)
                def _(source=source):
                    copy_from(source, p, chunk).start()

    def wait_chunk(chunk):
        for p in range(SLOTS):
            copy_from(partner_ref, p, chunk).wait()

    starts = []
    for p in range(SLOTS):
        side = fields[p, 3]
        starts.append(jnp.where(side == 0, fields[p, 4], EDGE * rank_of(fields, p, side)))
    xy_stages(
        [blocks.at[p] for p in range(SLOTS)],
        wait_chunk,
        starts,
        x_table_ref,
        y_table_ref,
        masked,
        grid_b,
    )
    z_stage(grid_b, column)
    lane = lax.broadcasted_iota(jnp.int32, (ROWS, LANES), 1)
    row = lax.broadcasted_iota(jnp.int32, (ROWS, LANES), 0)
    lane_zero, row_zero = lane % HALF == 0, row == 0
    total = cross_pass(grid_a, grid_b, sizes, lane_zero, row_zero)
    floor = jnp.zeros((1, LANES), F32)
    for p in range(SLOTS):
        mine = lane // HALF == p
        whole = jnp.sum(jnp.where(mine, total, 0.0), axis=(0, 1), keepdims=True)
        floor = jnp.where(mine[:1], whole * (2.0 / EDGE**3) + EPSILON, floor)
    floor = jnp.broadcast_to(floor, (ROWS, LANES))
    ratio_pass(grid_b, sizes, floor, lane_zero, row_zero)
    values = window_sums(grid_b, vy_ref, vz_ref, vx_ref)
    for p, line in enumerate(flattened(values, flat_ref)):
        corr_ref[p : p + 1, :] = line
    weight = values * values
    at = lax.broadcasted_iota(jnp.int32, (WIN * WIN, LANES), 0)
    along = [(at // WIN).astype(F32), (at % WIN).astype(F32)]
    k_row = (lane[:1] % WIN).astype(F32)
    plain = jnp.sum(weight, axis=0, keepdims=True)
    sums = [plain] + [jnp.sum(weight * a, axis=0, keepdims=True) for a in along] + [plain * k_row]
    stats = jnp.concatenate(sums + [jnp.zeros((ROWS - 4, LANES), F32)], axis=0) * (1.0 / WIN**3)
    for amount in (1, 2, 4):
        stats = stats + pltpu.roll(stats, LANES - amount, 1)
    shift_out = jnp.zeros((ROWS, LANES), F32)
    part = jnp.zeros((ROWS, LANES), F32)
    normal_lane = lane < 16
    first_of = jnp.where(normal_lane, lane // 4, lane % 4)
    second_of = jnp.where(normal_lane, lane % 4, (lane - 16) // 4)
    edge = float(EDGE)
    slab = lax.axis_index("slab").astype(F32)
    slab_height = (slab * edge + 0.5 * edge) / (edge * lax.axis_size("slab"))
    for p in range(SLOTS):
        energy = stats[0:1, p * WIN : p * WIN + 1]
        moved = []
        for axis in range(3):
            first_moment = stats[axis + 1 : axis + 2, p * WIN : p * WIN + 1]
            moment = first_moment + energy * fields[p, 5 + axis].astype(F32)
            moved.append(moment / (energy + EPSILON))
        anchor = (fields[p, 1].astype(F32) + 0.5 * edge) / (2.0 * edge)

        def center(index):
            last = jnp.where(index == 2, anchor, 1.0)
            return jnp.where(index == 0, slab_height, jnp.where(index == 1, 0.5, last))

        moved_lane = jnp.where(
            second_of == 0, moved[0], jnp.where(second_of == 1, moved[1], moved[2])
        )
        other = jnp.where(normal_lane, center(second_of), moved_lane)
        hit_a = (row == fields[p, 0]).astype(F32)
        hit_b = (row == fields[p, 2]).astype(F32)
        hits = jnp.where(normal_lane, hit_a + hit_b, hit_a - hit_b)
        part = part + hits * (energy * center(first_of) * other)
        for axis in range(3):
            shift_out = jnp.where((lane == p) & (row == axis), moved[axis], shift_out)
    shift_ref[...] = shift_out[:3, :SLOTS]
    part_ref[...] = jnp.where(lane < 28, part, 0.0)


def pick_view(fields, direction, rank):
    view = jnp.int32(0)
    seen = jnp.int32(0)
    for slot in range(SLOTS):
        asked = fields[slot, 3] == direction
        view = jnp.where(asked & (seen == rank), fields[slot, 2], view)
        seen = seen + asked.astype(jnp.int32)
    return view


def pick_start(fields, direction, rank):
    start = jnp.int32(0)
    seen = jnp.int32(0)
    for slot in range(SLOTS):
        asked = fields[slot, 3] == direction
        start = jnp.where(asked & (seen == rank), fields[slot, 4], start)
        seen = seen + asked.astype(jnp.int32)
    return start


def pack_kernel(toward, fields, volumes_ref, out_ref, held, sems):
    lane = lax.broadcasted_iota(jnp.int32, (EDGE, LANES), 1)
    low_half = lane < EDGE
    way = toward * partner_way()
    views = [pick_view(fields, way, rank) for rank in range(2)]

    def copy(n, chunk):
        return pltpu.make_async_copy(
            volumes_ref.at[views[n], pl.ds(chunk * PCHUNK, PCHUNK)],
            held.at[n, pl.ds(chunk * PCHUNK, PCHUNK)],
            sems.at[n, chunk],
        )

    for chunk in range(EDGE // PCHUNK):
        for n in range(2):
            copy(n, chunk).start()

    def weight(keep):
        return jnp.where(keep, 1.0, 0.0).astype(BF16)

    start_first, start_second = pick_start(fields, way, 0), pick_start(fields, way, 1)
    stay_first = weight(low_half & (lane >= start_first))
    stay_second = weight(~low_half & (lane < start_second + EDGE))
    move_first = weight(~low_half & (lane < start_first + EDGE))
    move_second = weight(low_half & (lane >= start_second))

    def step(chunk, carry):
        for n in range(2):
            copy(n, chunk).wait()
        for k in range(PCHUNK):
            z = chunk * PCHUNK + k
            first, second = held[0, z], held[1, z]
            moved = pltpu.roll(first * move_first + second * move_second, EDGE, 1)
            out_ref[z] = first * stay_first + second * stay_second + moved
        return carry

    lax.fori_loop(0, EDGE // PCHUNK, step, 0)


def packed_blocks(volumes, fields, toward):
    whole = pl.BlockSpec(memory_space=pltpu.VMEM)
    return pl.pallas_call(
        functools.partial(pack_kernel, toward),
        out_shape=pltpu.VMEM((EDGE, EDGE, LANES), BF16),
        in_specs=[pl.BlockSpec(memory_space=pltpu.SMEM), pl.BlockSpec(memory_space=pl.ANY)],
        out_specs=whole,
        scratch_shapes=[
            pltpu.VMEM((2, EDGE, EDGE, LANES), BF16),
            pltpu.SemaphoreType.DMA((2, EDGE // PCHUNK)),
        ],
        compiler_params=pltpu.CompilerParams(vmem_limit_bytes=GRANT),
    )(fields, volumes)


def first_spectra(volumes, pair_fields, x_tables, y_table):
    whole = pl.BlockSpec(memory_space=pltpu.VMEM)
    return pl.pallas_call(
        first_kernel,
        out_shape=pltpu.VMEM((EDGE, EDGE, 2 * LANES), F32),
        in_specs=[
            pl.BlockSpec(memory_space=pltpu.SMEM),
            pl.BlockSpec(memory_space=pl.ANY),
            whole,
            whole,
        ],
        out_specs=whole,
        scratch_shapes=[
            pltpu.VMEM((SLOTS, EDGE, EDGE, LANES), BF16),
            pltpu.VMEM((2, EDGE, ROWS, LANES), F32),
            pltpu.VMEM((2, 2 * LANES, 2 * LANES), BF16),
            pltpu.SemaphoreType.DMA((SLOTS, EDGE // XCHUNK)),
        ],
        compiler_params=pltpu.CompilerParams(vmem_limit_bytes=GRANT),
        name="first_spectra",
    )(pair_fields, volumes, x_tables, y_table)


def correlated(volumes, from_partner, from_cross, grid_a, pair_fields, tables):
    whole = pl.BlockSpec(memory_space=pltpu.VMEM)
    scalar = pl.BlockSpec(memory_space=pltpu.SMEM)
    left = pl.BlockSpec(memory_space=pl.ANY)
    return pl.pallas_call(
        second_kernel,
        out_shape=(
            jax.ShapeDtypeStruct((SLOTS, WIN**3), F32),
            jax.ShapeDtypeStruct((3, SLOTS), F32),
            jax.ShapeDtypeStruct((ROWS, LANES), F32),
        ),
        in_specs=[scalar] + [left] * 3 + [whole] * 7,
        out_specs=(whole,) * 3,
        scratch_shapes=[
            pltpu.VMEM((SLOTS, EDGE, EDGE, LANES), BF16),
            pltpu.VMEM((EDGE, EDGE, 2 * LANES), F32),
            pltpu.VMEM((HALF, 4, 4, ROWS, LANES), F32),
            pltpu.VMEM((2, EDGE, ROWS, LANES), F32),
            pltpu.VMEM((2, 2 * LANES, 2 * LANES), BF16),
            pltpu.SemaphoreType.DMA((SLOTS, EDGE // XCHUNK)),
        ],
        compiler_params=pltpu.CompilerParams(vmem_limit_bytes=GRANT),
        name="correlated",
    )(pair_fields, volumes, from_partner, from_cross, grid_a, *tables)


def split_outside(values):
    high = lax.reduce_precision(values, 8, 7)
    return high.astype(BF16), (values - high).astype(BF16)


def window_tables(pair_fields, pair_counts):
    slot = jnp.arange(EDGE, dtype=jnp.int32)
    freq = jnp.where(slot <= HALF, slot, slot - HALF)
    steps = jnp.arange(WIN, dtype=jnp.int32)
    shift = pair_fields[:, 1:2] - pair_fields[:, 4:5]
    offsets = pair_fields[:, 5:8] + jnp.where(jnp.arange(3) == 2, shift, 0)
    where_at = jnp.transpose(offsets)[:, :, None, None] + steps[None, None, :, None]
    phase = jnp.mod(where_at * freq, EDGE) - jnp.where(slot <= HALF, 0, EDGE // 4)
    values = jnp.cos((2.0 * math.pi / EDGE) * phase.astype(F32))
    vz = jnp.repeat(jnp.transpose(values[0], (2, 1, 0)), HALF, axis=2)
    high, low = split_outside(values[1].reshape(SLOTS * WIN, EDGE))
    vy = jnp.concatenate(
        [
            jnp.concatenate([high, high], axis=1),
            jnp.concatenate([low, jnp.zeros_like(low)], axis=1),
        ],
        axis=0,
    )
    live = (jnp.arange(SLOTS) < pair_counts[0]).astype(F32) * (2.0 / EDGE**1.5)
    vx = values[2] * live[:, None, None]
    vx = jnp.transpose(vx.reshape(SLOTS, WIN, 2, HALF), (2, 0, 3, 1))
    own = jnp.eye(SLOTS, dtype=F32)
    vx = (vx[:, :, :, None, :] * own[None, :, None, :, None]).reshape(2 * LANES, SLOTS * WIN)
    vx = jnp.pad(vx, ((0, 0), (0, LANES - SLOTS * WIN)))
    high, low = split_outside(vx)
    return vy, vz, jnp.concatenate([high, high, low], axis=0)


def groups_of(count, size, stride):
    return [
        [base + first + stride * k for k in range(size)]
        for base in range(0, count, size * stride)
        for first in range(stride)
    ]


def slab_total(part, axis):
    count = lax.axis_size(axis)
    reach = 1
    for size in (2, 4):
        if count % (reach * size):
            break
        groups = groups_of(count, size, reach)
        if size == 2:
            part = jnp.sum(
                lax.all_gather(part, axis, axis=0, tiled=False, axis_index_groups=groups), axis=0
            )
        else:
            part = lax.psum(part, axis, axis_index_groups=groups)
        reach *= size
    if reach < count:
        part = lax.psum(part, axis, axis_index_groups=groups_of(count, count // reach, reach))
    return part


def on_device(volumes, pair_fields, pair_counts):
    view_count = volumes.shape[0]
    slab_count = lax.axis_size("slab")
    volumes = pltpu.with_memory_space_constraint(volumes, pltpu.HBM)
    pair_fields = jnp.transpose(pair_fields)
    cross_fields = swapped(pair_fields, "slab", 1)
    partner_fields = swapped(pair_fields, "slab", 0)
    for_cross = packed_blocks(volumes, cross_fields, 1)
    from_cross = swapped(for_cross, "slab", 1)
    from_cross = pltpu.with_memory_space_constraint(from_cross, pltpu.HBM)
    partner_fields, for_cross = lax.optimization_barrier((partner_fields, for_cross))
    for_partner = packed_blocks(volumes, partner_fields, -1)
    from_partner = pltpu.with_memory_space_constraint(swapped(for_partner, "slab", 0), pltpu.HBM)
    late_fields, late_counts, for_partner = lax.optimization_barrier(
        (pair_fields, pair_counts, for_partner)
    )
    x_tables, y_table = jnp.asarray(x_tables_np()), jnp.asarray(y_table_np())
    grid_a = first_spectra(volumes, late_fields, x_tables, y_table)
    windows = window_tables(late_fields, late_counts)
    corr, shift, part = correlated(
        volumes,
        from_partner,
        from_cross,
        grid_a,
        late_fields,
        (x_tables, y_table, *windows, jnp.asarray(flat_table_np())),
    )
    part = jnp.transpose(slab_total(part, "slab") * (1.0 / (SLOTS * slab_count)))
    normal = jnp.transpose(part[:16, :view_count].reshape(4, 4, view_count), (2, 0, 1))
    rhs = jnp.transpose(part[16:28, :view_count].reshape(3, 4, view_count), (2, 1, 0))
    return corr, shift, normal, rhs


def solution(mesh):
    in_specs = (P("tm", "slab", None, None), P(None, ("tm", "slab")), P(("tm", "slab")))
    out_specs = (
        P(("tm", "slab"), None),
        P(None, ("tm", "slab")),
        P("tm", None, None),
        P("tm", None, None),
    )

    return jax.shard_map(
        on_device, mesh=mesh, in_specs=in_specs, out_specs=out_specs, check_vma=False
    )
```
